16 devices in a mesh: sp: 16 (over z, y, x, core).
Axes of the slice: x: 2, y: 2, z: 2, core: 2. Of those that a mesh axis runs over, the one named last changes fastest.
Arguments:
- x: bfloat16 [4, 2048, 2560], P(None, 'sp')
- ln1_w: bfloat16 [2560], replicated
- w_qkv: bfloat16 [2560, 7680], replicated
- q_ln_w: bfloat16 [32, 80], replicated
- k_ln_w: bfloat16 [32, 80], replicated
- w_out: bfloat16 [2560, 2560], replicated
- grad_y: bfloat16 [4, 2048, 2560], P(None, 'sp')
Outputs:
- output 1: bfloat16 [4, 2048, 2560], P(None, 'sp')
- output 2: bfloat16 [4, 2048, 2560], P(None, 'sp')
- output 3: float32 [2560], replicated
- output 4: float32 [2560, 7680], replicated
- output 5: float32 [32, 80], replicated
- output 6: float32 [32, 80], replicated
- output 7: float32 [2560, 2560], replicated
All inputs are finite; a program needn't handle non-finite values.
Results may differ from the reference program's by a relative error of at most 0.0121307.
Values are sent between devices in bfloat16 or wider.
A program may use at most 1 GiB of HBM per device.

```python
import math
import jax
import jax.numpy as jnp
from jax import lax

BATCH_SIZE = 4
SEQ_LEN = 2048
D_MODEL = 2560
N_HEADS = 32
HEAD_DIM = 80
Q_BLOCK = math.gcd(SEQ_LEN, 256)


def alibi_slopes(n_heads):
    pow_two = 2 ** math.ceil(math.log2(n_heads))
    exponents = jnp.arange(1, pow_two + 1, dtype=jnp.float32) * (8.0 / pow_two)
    slopes = jnp.exp2(-exponents)
    if pow_two != n_heads:
        slopes = jnp.concatenate([slopes[1::2], slopes[0::2]])[:n_heads]
    return slopes


def layer_norm(values, weight):
    centered = values - jnp.mean(values, axis=-1, keepdims=True)
    var_val = jnp.mean(centered * centered, axis=-1, keepdims=True)
    return centered * lax.rsqrt(var_val + 1e-5) * weight


def bf_cast(values):
    return values.astype(jnp.bfloat16).astype(jnp.float32)


def setup_inputs(seed: int = 0) -> dict:
    key_list = jax.random.split(jax.random.key(seed), 8)
    act_shape = (BATCH_SIZE, SEQ_LEN, D_MODEL)
    w_scale = D_MODEL ** -0.5
    head_gain = jnp.exp2(jax.random.uniform(key_list[3], (N_HEADS, 1), jnp.float32, -1.0, 1.0))
    q_gain = (1.0 + 0.3 * jax.random.normal(key_list[4], (N_HEADS, HEAD_DIM), jnp.float32)) * head_gain
    return {
        'x': jax.random.normal(key_list[0], act_shape, jnp.float32).astype(jnp.bfloat16),
        'ln1_w': (1.0 + 0.3 * jax.random.normal(key_list[1], (D_MODEL,), jnp.float32)).astype(jnp.bfloat16),
        'w_qkv': (jax.random.normal(key_list[2], (D_MODEL, 3 * D_MODEL), jnp.float32) * w_scale).astype(jnp.bfloat16),
        'q_ln_w': q_gain.astype(jnp.bfloat16),
        'k_ln_w': (1.0 + 0.3 * jax.random.normal(key_list[5], (N_HEADS, HEAD_DIM), jnp.float32)).astype(jnp.bfloat16),
        'w_out': (jax.random.normal(key_list[6], (D_MODEL, D_MODEL), jnp.float32) * w_scale).astype(jnp.bfloat16),
        'grad_y': jax.random.normal(key_list[7], act_shape, jnp.float32).astype(jnp.bfloat16),
    }


def head_attention(head_args):
    q_head, k_head, v_head, head_slope = head_args
    key_pos = jnp.arange(SEQ_LEN)

    def block_attention(blk_idx):
        q_part = lax.dynamic_slice_in_dim(q_head, blk_idx * Q_BLOCK, Q_BLOCK, axis=1)
        scores = jnp.einsum('bqd,bkd->bqk', q_part, k_head) * (HEAD_DIM ** -0.5)
        pos_gap = (blk_idx * Q_BLOCK + jnp.arange(Q_BLOCK))[:, None] - key_pos[None, :]
        scores = jnp.where(pos_gap >= 0, scores - head_slope * pos_gap.astype(jnp.float32), -1e30)
        row_max = lax.stop_gradient(jnp.max(scores, axis=-1, keepdims=True))
        weights = jnp.exp(scores - row_max)
        weighted = jnp.einsum('bqk,bkd->bqd', weights, v_head)
        return weighted / jnp.sum(weights, axis=-1, keepdims=True)

    out_blocks = lax.map(jax.checkpoint(block_attention), jnp.arange(SEQ_LEN // Q_BLOCK))
    return jnp.moveaxis(out_blocks, 0, 1).reshape(BATCH_SIZE, SEQ_LEN, HEAD_DIM)


def forward_pass(x, ln1_w, w_qkv, q_ln_w, k_ln_w, w_out):
    h_act = bf_cast(layer_norm(x, ln1_w))
    qkv_raw = jnp.einsum('bsd,de->bse', h_act, w_qkv)
    q_all = bf_cast(layer_norm(qkv_raw[..., :D_MODEL], q_ln_w.reshape(D_MODEL)))
    k_all = bf_cast(layer_norm(qkv_raw[..., D_MODEL:2 * D_MODEL], k_ln_w.reshape(D_MODEL)))
    v_all = bf_cast(qkv_raw[..., 2 * D_MODEL:])
    head_shape = (BATCH_SIZE, SEQ_LEN, N_HEADS, HEAD_DIM)
    per_head = [jnp.moveaxis(tensor.reshape(head_shape), 2, 0) for tensor in (q_all, k_all, v_all)]
    o_heads = lax.map(jax.checkpoint(head_attention), (per_head[0], per_head[1], per_head[2], alibi_slopes(N_HEADS)))
    o_all = bf_cast(jnp.moveaxis(o_heads, 0, 2).reshape(BATCH_SIZE, SEQ_LEN, D_MODEL))
    return jnp.einsum('bsd,de->bse', o_all, w_out) + x


def reference(x, ln1_w, w_qkv, q_ln_w, k_ln_w, w_out, grad_y):
    y_val, pull_back = jax.vjp(forward_pass, x.astype(jnp.float32), ln1_w.astype(jnp.float32), w_qkv.astype(jnp.float32), q_ln_w.astype(jnp.float32), k_ln_w.astype(jnp.float32), w_out.astype(jnp.float32))
    grad_list = pull_back(grad_y.astype(jnp.float32))
    return (y_val.astype(jnp.bfloat16), grad_list[0].astype(jnp.bfloat16), grad_list[1], grad_list[2], grad_list[3], grad_list[4], grad_list[5])
```

```python
import functools
import math
import jax
import jax.numpy as jnp
from jax import lax
from jax.experimental import pallas as pl
from jax.experimental.pallas import tpu as pltpu
from jax.sharding import PartitionSpec as P

F32 = jnp.float32
BF16 = jnp.bfloat16
LANES = 128
LOG2E = math.log2(math.e)
MESH = pl.DeviceIdType.MESH


def alibi_slopes(n_heads):
    pow_two = 2 ** math.ceil(math.log2(n_heads))
    exponents = jnp.arange(1, pow_two + 1, dtype=F32) * (8.0 / pow_two)
    slopes = jnp.exp2(-exponents)
    if pow_two != n_heads:
        slopes = jnp.concatenate([slopes[1::2], slopes[0::2]])[:n_heads]
    return slopes


def layer_norm(values, weight):
    centered = values - jnp.mean(values, axis=-1, keepdims=True)
    var_val = jnp.mean(centered * centered, axis=-1, keepdims=True)
    return centered * lax.rsqrt(var_val + 1e-5) * weight


def row_stats(values):
    mean = jnp.mean(values, axis=-1, keepdims=True)
    centered = values - mean
    var_val = jnp.mean(centered * centered, axis=-1)
    return mean[..., 0], lax.rsqrt(var_val + 1e-5)


def exchange(block, n_dev):
    def kernel(x_ref, o_ref, loc_sem, send_sem, recv_sem):
        me = lax.axis_index('sp')
        own = pltpu.make_async_copy(x_ref, o_ref.at[me], loc_sem)
        own.start()
        copies = []
        for step in range(1, n_dev):
            copies.append(pltpu.make_async_remote_copy(
                src_ref=x_ref, dst_ref=o_ref.at[me], send_sem=send_sem.at[step], recv_sem=recv_sem.at[step],
                device_id=(lax.rem(me + step, n_dev),), device_id_type=MESH))
            copies[-1].start()
        own.wait()
        for copy in copies:
            copy.wait()

    return pl.pallas_call(
        kernel,
        out_shape=jax.ShapeDtypeStruct((n_dev,) + block.shape, block.dtype),
        in_specs=[pl.BlockSpec(memory_space=pl.ANY)],
        out_specs=pl.BlockSpec(memory_space=pl.ANY),
        scratch_shapes=[pltpu.SemaphoreType.DMA, pltpu.SemaphoreType.DMA((n_dev,)), pltpu.SemaphoreType.DMA((n_dev,))],
        compiler_params=pltpu.CompilerParams(has_side_effects=True),
        name='exchange',
    )(block)


def qkv_heads(h_all, w_pad, stats, gains, n_dev, n_batch, tok, seq):
    rows = n_batch * tok
    d_model = h_all.shape[-1]
    n_h = gains.shape[0] // 2

    def kernel(h_ref, w_ref, st_ref, g_ref, q_ref, k_ref, v_ref, xq_ref, xk_ref):
        raw = jnp.dot(h_ref[...], w_ref[...], preferred_element_type=F32)
        st = st_ref[...]
        for n in range(n_h):
            for part, (o_ref, x_ref) in enumerate(((q_ref, xq_ref), (k_ref, xk_ref))):
                col = (part * n_h + n) * LANES
                hat = (raw[:, col:col + LANES] - st[:, 2 * part:2 * part + 1]) * st[:, 2 * part + 1:2 * part + 2]
                out = (hat * g_ref[part * n_h + n:part * n_h + n + 1, :]).astype(BF16)
                x_ref[:, n] = hat.reshape(n_batch, tok, LANES)
                o_ref[:, n] = out.reshape(n_batch, tok, LANES)
            col = (2 * n_h + n) * LANES
            v_ref[:, n] = raw[:, col:col + LANES].astype(BF16).reshape(n_batch, tok, LANES)

    shape = (n_batch, n_h, seq, LANES)
    spec = pl.BlockSpec((n_batch, n_h, tok, LANES), lambda i: (0, 0, i, 0))
    n_col = w_pad.shape[1]
    return pl.pallas_call(
        kernel,
        grid=(n_dev,),
        out_shape=[jax.ShapeDtypeStruct(shape, BF16)] * 3 + [jax.ShapeDtypeStruct(shape, F32)] * 2,
        in_specs=[pl.BlockSpec((rows, d_model), lambda i: (i, 0)), pl.BlockSpec((d_model, n_col), lambda i: (0, 0)),
                  pl.BlockSpec((rows, stats.shape[1]), lambda i: (i, 0)), pl.BlockSpec(gains.shape, lambda i: (0, 0))],
        out_specs=[spec] * 5,
        compiler_params=pltpu.CompilerParams(vmem_limit_bytes=60 * 2 ** 20),
        cost_estimate=pl.CostEstimate(flops=2 * n_dev * rows * d_model * n_col, bytes_accessed=80 * 2 ** 20, transcendentals=0),
        name='qkv_heads',
    )(h_all, w_pad, stats, gains)


def attention(q, k, v, d_o, slopes, head_dim, blk):
    n_batch, n_h, seq, _ = q.shape
    n_blk = seq // blk
    scale = head_dim ** -0.5

    def dot(a, b, ca, cb):
        return lax.dot_general(a, b, (((ca,), (cb,)), ((), ())), preferred_element_type=F32)

    def kernel(slope_ref, q_ref, k_ref, v_ref, do_ref, o_ref, dq_ref, dk_ref, dv_ref, s_ref, dk_acc, dv_acc):
        slope2 = slope_ref[pl.program_id(1)] * LOG2E
        dk_acc[...] = jnp.zeros_like(dk_acc)
        dv_acc[...] = jnp.zeros_like(dv_acc)
        key_iota = lax.broadcasted_iota(jnp.int32, (blk, LANES), 0)[:, :1]

        @pl.loop(0, n_blk)
        def _(i):
            q_rows = pl.ds(i * blk, blk)
            q_b = q_ref[0, 0, q_rows, :]
            do_b = do_ref[0, 0, q_rows, :]

            def score(j, diag):
                rows = pl.ds(j * blk, blk)
                s = dot(k_ref[0, 0, rows, :], q_b, 1, 1) * (scale * LOG2E)
                s = s + (key_iota + (j - i) * blk).astype(F32) * slope2
                if diag:
                    key_pos = lax.broadcasted_iota(jnp.int32, (blk, blk), 0)
                    q_pos = lax.broadcasted_iota(jnp.int32, (blk, blk), 1)
                    s = jnp.where(key_pos <= q_pos, s, -1e30)
                s_ref[rows, :] = s
                return jnp.max(s, axis=0, keepdims=True)

            top = score(i, True)
            top = lax.fori_loop(0, i, lambda j, m: jnp.maximum(m, score(j, False)), top)

            def weigh(j, carry):
                total, out_t = carry
                rows = pl.ds(j * blk, blk)
                w = jnp.exp2(s_ref[rows, :] - top)
                s_ref[rows, :] = w
                out_t = out_t + dot(v_ref[0, 0, rows, :], w.astype(BF16), 0, 0)
                return total + jnp.sum(w, axis=0, keepdims=True), out_t

            total, out_t = lax.fori_loop(0, i + 1, weigh, (jnp.zeros((1, blk), F32), jnp.zeros((LANES, blk), F32)))
            inv = 1.0 / total
            out_b = (out_t * inv).T.astype(BF16)
            o_ref[0, 0, q_rows, :] = out_b
            delta = jnp.sum((out_b.astype(F32) * do_b.astype(F32)).T, axis=0, keepdims=True)

            def back(j, dq_t):
                rows = pl.ds(j * blk, blk)
                k_b = k_ref[0, 0, rows, :]
                d_p = dot(v_ref[0, 0, rows, :], do_b, 1, 1)
                p = s_ref[rows, :] * inv
                dv_acc[rows, :] += dot(p.astype(BF16), do_b, 1, 0)
                d_s = (p * (d_p - delta)).astype(BF16)
                dk_acc[rows, :] += dot(d_s, q_b, 1, 0)
                return dq_t + dot(k_b, d_s, 0, 0)

            dq_t = lax.fori_loop(0, i + 1, back, jnp.zeros((LANES, blk), F32))
            dq_ref[0, 0, q_rows, :] = (dq_t * scale).T.astype(BF16)

        dk_ref[0, 0] = (dk_acc[...] * scale).astype(BF16)
        dv_ref[0, 0] = dv_acc[...].astype(BF16)

    spec = pl.BlockSpec((1, 1, seq, LANES), lambda b, n: (b, n, 0, 0))
    flops = 6 * 2 * n_batch * n_h * seq * seq * LANES
    return pl.pallas_call(
        kernel,
        grid=(n_batch, n_h),
        out_shape=[jax.ShapeDtypeStruct(q.shape, BF16)] * 4,
        in_specs=[pl.BlockSpec(memory_space=pltpu.SMEM)] + [spec] * 4,
        out_specs=[spec] * 4,
        scratch_shapes=[pltpu.VMEM((seq, blk), F32), pltpu.VMEM((seq, LANES), F32), pltpu.VMEM((seq, LANES), F32)],
        compiler_params=pltpu.CompilerParams(vmem_limit_bytes=60 * 2 ** 20),
        cost_estimate=pl.CostEstimate(flops=flops, bytes_accessed=40 * 2 ** 20, transcendentals=n_batch * n_h * seq * seq // 2),
        name='attention',
    )(slopes, q, k, v, d_o)


def place_columns(gathered, group):
    n_dev, parts, width, d_in = gathered.shape
    mb = 512 if d_in % 512 == 0 else d_in

    def kernel(x_ref, o_ref):
        o_ref[...] = x_ref[...].reshape(group * width, mb).T

    n_grp = n_dev // group
    return pl.pallas_call(
        kernel,
        grid=(parts, n_grp, d_in // mb),
        out_shape=jax.ShapeDtypeStruct((d_in, parts * n_dev * width), gathered.dtype),
        in_specs=[pl.BlockSpec((group, 1, width, mb), lambda p, g, m: (g, p, 0, m))],
        out_specs=pl.BlockSpec((mb, group * width), lambda p, g, m: (m, p * n_grp + g)),
        compiler_params=pltpu.CompilerParams(vmem_limit_bytes=40 * 2 ** 20),
        cost_estimate=pl.CostEstimate(flops=2 * gathered.size, bytes_accessed=8 * gathered.size, transcendentals=0),
        name='place_columns',
    )(gathered)


def solution(mesh):
    n_dev = mesh.shape['sp']
    seq_spec = P(None, 'sp', None)
    rep_spec = P()

    def local_step(x, ln1_w, w_qkv, q_ln_w, k_ln_w, w_out, grad_y):
        n_batch, tok, d_model = x.shape
        n_heads, head_dim = q_ln_w.shape
        n_h = n_heads // n_dev
        width = n_h * head_dim
        seq = tok * n_dev
        rows = n_batch * tok
        me = lax.axis_index('sp')
        slopes = lax.dynamic_slice_in_dim(alibi_slopes(n_heads), me * n_h, n_h)

        def pad_lanes(a):
            return jnp.pad(a, ((0, 0),) * (a.ndim - 1) + ((0, LANES - head_dim),))

        x_flat = x.reshape(rows, d_model).astype(F32)
        gy = grad_y.reshape(rows, d_model)
        h_f32, ln1_pull = jax.vjp(layer_norm, x_flat, ln1_w.astype(F32))
        h_loc = h_f32.astype(BF16)
        h_all = lax.all_gather(h_loc, 'sp', axis=0, tiled=True)

        qk_raw = jnp.dot(h_loc, w_qkv[:, :2 * d_model], preferred_element_type=F32)
        stats_loc = jnp.stack(row_stats(qk_raw[:, :d_model]) + row_stats(qk_raw[:, d_model:]))
        stats = exchange(stats_loc, n_dev)
        d_o = jnp.einsum('te,nde->ntd', gy, w_out.reshape(n_dev, width, d_model), preferred_element_type=F32).astype(BF16)
        d_o = lax.all_to_all(d_o, 'sp', 0, 0, tiled=True)
        d_o = d_o.reshape(n_dev, n_batch, tok, n_h, head_dim).transpose(1, 3, 0, 2, 4).reshape(n_batch, n_h, seq, head_dim)
        d_o = pad_lanes(d_o)
        slices = [lax.dynamic_slice_in_dim(w_qkv, p * d_model + me * width, width, axis=1) for p in range(3)]
        w_pad = jnp.concatenate([pad_lanes(s[:, n * head_dim:(n + 1) * head_dim]) for s in slices for n in range(n_h)], axis=1)
        gain_q = pad_lanes(lax.dynamic_slice_in_dim(q_ln_w, me * n_h, n_h).astype(F32))
        gain_k = pad_lanes(lax.dynamic_slice_in_dim(k_ln_w, me * n_h, n_h).astype(F32))
        stats_rows = stats.transpose(0, 2, 1).reshape(n_dev * rows, 4)

        q, k, v, hat_q, hat_k = qkv_heads(h_all, w_pad, stats_rows, jnp.concatenate([gain_q, gain_k]), n_dev, n_batch, tok, seq)
        gy_late, h_all = lax.optimization_barrier((gy, h_all))
        gy_all = lax.all_gather(gy_late, 'sp', axis=0, tiled=True)
        o, d_q, d_k, d_v = attention(q, k, v, d_o, slopes, head_dim, math.gcd(seq, 512))

        rstd = stats.reshape(n_dev, 4, n_batch, tok).transpose(1, 2, 0, 3).reshape(4, n_batch, seq)
        dq32, dk32 = d_q.astype(F32), d_k.astype(F32)
        gq = dq32 * gain_q[None, :, None, :]
        gk = dk32 * gain_k[None, :, None, :]
        part = jnp.stack([jnp.sum(gq, (1, 3)), jnp.sum(gq * hat_q, (1, 3)), jnp.sum(gk, (1, 3)), jnp.sum(gk * hat_k, (1, 3))])
        full = jnp.sum(exchange(part.reshape(-1, LANES), n_dev), axis=0).reshape(4, n_batch, seq) * (1.0 / d_model)

        def norm_back(g, hat, c1, c2, r):
            e = lambda a: a[:, None, :, None]
            return (e(r) * (g - e(c1) - hat * e(c2))).astype(BF16)

        dq_raw = norm_back(gq, hat_q, full[0], full[1], rstd[1])
        dk_raw = norm_back(gk, hat_k, full[2], full[3], rstd[3])
        grad_q_ln = jnp.sum(dq32 * hat_q, (0, 2))[:, :head_dim]
        grad_k_ln = jnp.sum(dk32 * hat_k, (0, 2))[:, :head_dim]

        def to_rows(a):
            a = a[..., :head_dim].reshape(n_batch, n_h, n_dev, tok, head_dim)
            return a.transpose(2, 0, 3, 1, 4).reshape(n_dev, rows, width)

        back = jnp.concatenate([to_rows(a) for a in (dq_raw, dk_raw, d_v, o)], axis=-1)
        back_flat = back.reshape(n_dev * rows, 4 * width)
        tok_side = lax.all_to_all(back, 'sp', 0, 0, tiled=True)
        dw_out = lax.dot_general(back_flat[:, 3 * width:], gy_all, (((0,), (0,)), ((), ())), preferred_element_type=F32)
        dw_qkv_t = lax.dot_general(back_flat[:, :3 * width], h_all, (((0,), (0,)), ((), ())), preferred_element_type=F32)
        grad_w_out = lax.all_gather(dw_out, 'sp', axis=0, tiled=True)
        dw_all = lax.all_gather(dw_qkv_t, 'sp', axis=0, tiled=True)
        grad_w_qkv = place_columns(dw_all.reshape(n_dev, 3, width, d_model), 4)

        o_tok = tok_side[:, :, 3 * width:].transpose(1, 0, 2).reshape(rows, d_model)
        y = (jnp.dot(o_tok, w_out, preferred_element_type=F32) + x_flat).astype(BF16)
        d_qkv = tok_side[:, :, :3 * width].reshape(n_dev, rows, 3, width).transpose(1, 2, 0, 3).reshape(rows, 3 * d_model)
        d_h = lax.dot_general(d_qkv, w_qkv, (((1,), (1,)), ((), ())), preferred_element_type=F32).astype(BF16)
        d_x_norm, grad_ln1 = ln1_pull(d_h.astype(F32))
        grad_x = (d_x_norm + gy.astype(F32)).astype(BF16)

        small = jnp.concatenate([grad_ln1, grad_q_ln.reshape(-1), grad_k_ln.reshape(-1)])
        n_small = small.shape[0]
        pad = -n_small % (8 * LANES)
        small_all = exchange(jnp.pad(small, (0, pad)).reshape(-1, LANES), n_dev).reshape(n_dev, n_small + pad)
        grad_ln1 = jnp.sum(small_all[:, :d_model], axis=0)
        grad_q_ln = small_all[:, d_model:d_model + width].reshape(n_heads, head_dim)
        grad_k_ln = small_all[:, d_model + width:d_model + 2 * width].reshape(n_heads, head_dim)
        shape = (n_batch, tok, d_model)
        return y.reshape(shape), grad_x.reshape(shape), grad_ln1, grad_w_qkv, grad_q_ln, grad_k_ln, grad_w_out

    return jax.shard_map(local_step, mesh=mesh, in_specs=(seq_spec, rep_spec, rep_spec, rep_spec, rep_spec, rep_spec, seq_spec), out_specs=(seq_spec, seq_spec, rep_spec, rep_spec, rep_spec, rep_spec, rep_spec), check_vma=False)
```

```python
import math
import jax
import jax.numpy as jnp
from jax import lax
from jax.experimental import pallas as pl
from jax.experimental.pallas import tpu as pltpu
from jax.sharding import PartitionSpec as P

F32 = jnp.float32
BF16 = jnp.bfloat16
LANES = 128
LOG2E = math.log2(math.e)
MESH = pl.DeviceIdType.MESH


def alibi_slopes(n_heads):
    pow_two = 2 ** math.ceil(math.log2(n_heads))
    exponents = jnp.arange(1, pow_two + 1, dtype=F32) * (8.0 / pow_two)
    slopes = jnp.exp2(-exponents)
    if pow_two != n_heads:
        slopes = jnp.concatenate([slopes[1::2], slopes[0::2]])[:n_heads]
    return slopes


def layer_norm(values, weight):
    centered = values - jnp.mean(values, axis=-1, keepdims=True)
    var_val = jnp.mean(centered * centered, axis=-1, keepdims=True)
    return centered * lax.rsqrt(var_val + 1e-5) * weight


def row_stats(values):
    mean = jnp.mean(values, axis=-1, keepdims=True)
    centered = values - mean
    var_val = jnp.mean(centered * centered, axis=-1)
    return mean[..., 0], lax.rsqrt(var_val + 1e-5)


def exchange(block, n_dev, scatter=False):
    shape = block.shape[1:] if scatter else block.shape

    def kernel(x_ref, o_ref, loc_sem, send_sem, recv_sem):
        me = lax.axis_index('sp')
        src = (lambda dev: x_ref.at[dev]) if scatter else (lambda dev: x_ref)
        own = pltpu.make_async_copy(src(me), o_ref.at[me], loc_sem)
        own.start()
        copies = []
        for step in range(1, n_dev):
            peer = lax.rem(me + step, n_dev)
            copies.append(pltpu.make_async_remote_copy(
                src_ref=src(peer), dst_ref=o_ref.at[me], send_sem=send_sem.at[step], recv_sem=recv_sem.at[step],
                device_id=(peer,), device_id_type=MESH))
            copies[-1].start()
        own.wait()
        for copy in copies:
            copy.wait()

    return pl.pallas_call(
        kernel,
        out_shape=jax.ShapeDtypeStruct((n_dev,) + shape, block.dtype),
        in_specs=[pl.BlockSpec(memory_space=pl.ANY)],
        out_specs=pl.BlockSpec(memory_space=pl.ANY),
        scratch_shapes=[pltpu.SemaphoreType.DMA, pltpu.SemaphoreType.DMA((n_dev,)), pltpu.SemaphoreType.DMA((n_dev,))],
        compiler_params=pltpu.CompilerParams(has_side_effects=True),
        name='scatter_rows' if scatter else 'exchange',
    )(block)


def qkv_heads(h_all, w_pad, stats, gains, n_dev, n_batch, tok, seq):
    rows = n_batch * tok
    d_model = h_all.shape[-1]
    n_h = gains.shape[0] // 2

    def kernel(h_ref, w_ref, st_ref, g_ref, q_ref, k_ref, v_ref, xq_ref, xk_ref):
        raw = jnp.dot(h_ref[...], w_ref[...], preferred_element_type=F32)
        st = st_ref[...]
        for n in range(n_h):
            for part, (o_ref, x_ref) in enumerate(((q_ref, xq_ref), (k_ref, xk_ref))):
                col = (part * n_h + n) * LANES
                hat = (raw[:, col:col + LANES] - st[:, 2 * part:2 * part + 1]) * st[:, 2 * part + 1:2 * part + 2]
                out = (hat * g_ref[part * n_h + n:part * n_h + n + 1, :]).astype(BF16)
                x_ref[:, n] = hat.reshape(n_batch, tok, LANES)
                o_ref[:, n] = out.reshape(n_batch, tok, LANES)
            col = (2 * n_h + n) * LANES
            v_ref[:, n] = raw[:, col:col + LANES].astype(BF16).reshape(n_batch, tok, LANES)

    shape = (n_batch, n_h, seq, LANES)
    spec = pl.BlockSpec((n_batch, n_h, tok, LANES), lambda i: (0, 0, i, 0))
    n_col = w_pad.shape[1]
    return pl.pallas_call(
        kernel,
        grid=(n_dev,),
        out_shape=[jax.ShapeDtypeStruct(shape, BF16)] * 3 + [jax.ShapeDtypeStruct(shape, F32)] * 2,
        in_specs=[pl.BlockSpec((rows, d_model), lambda i: (i, 0)), pl.BlockSpec((d_model, n_col), lambda i: (0, 0)),
                  pl.BlockSpec((rows, stats.shape[1]), lambda i: (i, 0)), pl.BlockSpec(gains.shape, lambda i: (0, 0))],
        out_specs=[spec] * 5,
        compiler_params=pltpu.CompilerParams(vmem_limit_bytes=60 * 2 ** 20),
        cost_estimate=pl.CostEstimate(flops=2 * n_dev * rows * d_model * n_col, bytes_accessed=80 * 2 ** 20, transcendentals=0),
        name='qkv_heads',
    )(h_all, w_pad, stats, gains)


def attention(q, k, v, d_o, slopes, head_dim, blk):
    n_batch, n_h, seq, _ = q.shape
    n_blk = seq // blk
    scale = head_dim ** -0.5

    def dot(a, b):
        return jnp.dot(a, b, preferred_element_type=F32)

    def kernel(slope_ref, q_ref, k_ref, v_ref, do_ref, o_ref, dq_ref, dk_ref, dv_ref, w_ref, dk_acc, dv_acc, kt_ref, vt_ref):
        slope2 = slope_ref[pl.program_id(1)] * LOG2E
        dk_acc[...] = jnp.zeros_like(dk_acc)
        dv_acc[...] = jnp.zeros_like(dv_acc)
        kt_ref[...] = k_ref[0, 0].T
        vt_ref[...] = v_ref[0, 0].T
        key_iota = lax.broadcasted_iota(jnp.int32, (blk, LANES), 0)[:, :1]
        blocks = [pl.ds(j * blk, blk) for j in range(n_blk)]

        for i in range(n_blk):
            q_b = q_ref[0, 0, blocks[i], :]
            do_b = do_ref[0, 0, blocks[i], :]
            q_t = q_b.T
            do_t = do_b.T
            top = None
            for j in range(i, -1, -1):
                s = dot(k_ref[0, 0, blocks[j], :], q_t) * (scale * LOG2E)
                s = s + (key_iota + (j - i) * blk).astype(F32) * slope2
                if i == j:
                    key_pos = lax.broadcasted_iota(jnp.int32, (blk, blk), 0)
                    q_pos = lax.broadcasted_iota(jnp.int32, (blk, blk), 1)
                    s = jnp.where(key_pos <= q_pos, s, -1e30)
                w_ref[blocks[j], :] = s
                peak = jnp.max(s, axis=0, keepdims=True)
                top = peak if top is None else jnp.maximum(top, peak)

            total = jnp.zeros((1, blk), F32)
            out_t = jnp.zeros((LANES, blk), F32)
            for j in range(i + 1):
                w = jnp.exp2(w_ref[blocks[j], :] - top)
                w_ref[blocks[j], :] = w
                out_t = out_t + dot(vt_ref[:, blocks[j]], w.astype(BF16))
                total = total + jnp.sum(w, axis=0, keepdims=True)
            inv = 1.0 / total
            out_b = (out_t * inv).T.astype(BF16)
            o_ref[0, 0, blocks[i], :] = out_b
            delta = jnp.sum((out_b.astype(F32) * do_b.astype(F32)).T, axis=0, keepdims=True)

            dq_t = jnp.zeros((LANES, blk), F32)
            for j in range(i + 1):
                d_p = dot(v_ref[0, 0, blocks[j], :], do_t)
                p = w_ref[blocks[j], :] * inv
                dv_acc[blocks[j], :] += dot(p.astype(BF16), do_b)
                d_s = (p * (d_p - delta)).astype(BF16)
                dk_acc[blocks[j], :] += dot(d_s, q_b)
                dq_t = dq_t + dot(kt_ref[:, blocks[j]], d_s)
            dq_ref[0, 0, blocks[i], :] = (dq_t * scale).T.astype(BF16)

        dk_ref[0, 0] = (dk_acc[...] * scale).astype(BF16)
        dv_ref[0, 0] = dv_acc[...].astype(BF16)

    spec = pl.BlockSpec((1, 1, seq, LANES), lambda b, n: (b, n, 0, 0))
    flops = 6 * 2 * n_batch * n_h * seq * seq * LANES
    return pl.pallas_call(
        kernel,
        grid=(n_batch, n_h),
        out_shape=[jax.ShapeDtypeStruct(q.shape, BF16)] * 4,
        in_specs=[pl.BlockSpec(memory_space=pltpu.SMEM)] + [spec] * 4,
        out_specs=[spec] * 4,
        scratch_shapes=[pltpu.VMEM((seq, blk), F32), pltpu.VMEM((seq, LANES), F32), pltpu.VMEM((seq, LANES), F32),
                        pltpu.VMEM((LANES, seq), BF16), pltpu.VMEM((LANES, seq), BF16)],
        compiler_params=pltpu.CompilerParams(vmem_limit_bytes=60 * 2 ** 20),
        cost_estimate=pl.CostEstimate(flops=flops, bytes_accessed=40 * 2 ** 20, transcendentals=n_batch * n_h * seq * seq // 2),
        name='attention',
    )(slopes, q, k, v, d_o)


def place_columns(buf, gathered, first, n_part, group):
    n_dev, parts, width, d_in = gathered.shape
    mb = 512 if d_in % 512 == 0 else d_in
    n_grp = n_dev // group

    def kernel(x_ref, *refs):
        refs[-1][...] = x_ref[...].reshape(group * width, mb).T

    args = (gathered,) if buf is None else (gathered, buf)
    return pl.pallas_call(
        kernel,
        grid=(parts, n_grp, d_in // mb),
        out_shape=jax.ShapeDtypeStruct((d_in, n_part * n_dev * width), gathered.dtype),
        in_specs=[pl.BlockSpec((group, 1, width, mb), lambda p, g, m: (g, p, 0, m))] + [pl.BlockSpec(memory_space=pl.ANY)] * (len(args) - 1),
        out_specs=pl.BlockSpec((mb, group * width), lambda p, g, m: (m, (p + first) * n_grp + g)),
        input_output_aliases={1: 0} if buf is not None else {},
        compiler_params=pltpu.CompilerParams(vmem_limit_bytes=40 * 2 ** 20),
        cost_estimate=pl.CostEstimate(flops=2 * gathered.size, bytes_accessed=8 * gathered.size, transcendentals=0),
        name='place_columns',
    )(*args)


def head_grads(side, acts, n_dev, n_batch, tok, head_dim):
    n_h = side.shape[1]
    rows, d_model = n_batch * tok, acts.shape[-1]

    def kernel(s_ref, a_ref, o_ref, acc):
        step = pl.program_id(0)
        lhs = jnp.concatenate([s_ref[:, n].reshape(rows, LANES) for n in range(n_h)], axis=1)
        out = lax.dot_general(lhs, a_ref[...], (((0,), (0,)), ((), ())), preferred_element_type=F32)

        @pl.when(step == 0)
        def _():
            acc[...] = out

        @pl.when(step > 0)
        def _():
            acc[...] += out

        @pl.when(step == n_dev - 1)
        def _():
            for n in range(n_h):
                o_ref[n * head_dim:(n + 1) * head_dim, :] = acc[n * LANES:n * LANES + head_dim, :]

    return pl.pallas_call(
        kernel,
        grid=(n_dev,),
        out_shape=jax.ShapeDtypeStruct((n_h * head_dim, d_model), F32),
        in_specs=[pl.BlockSpec((n_batch, n_h, tok, LANES), lambda i: (0, 0, i, 0)), pl.BlockSpec((rows, d_model), lambda i: (i, 0))],
        out_specs=pl.BlockSpec((n_h * head_dim, d_model), lambda i: (0, 0)),
        scratch_shapes=[pltpu.VMEM((n_h * LANES, d_model), F32)],
        compiler_params=pltpu.CompilerParams(vmem_limit_bytes=50 * 2 ** 20),
        cost_estimate=pl.CostEstimate(flops=2 * n_dev * rows * d_model * n_h * LANES, bytes_accessed=50 * 2 ** 20, transcendentals=0),
        name='head_grads',
    )(side, acts)


def norm_back(d_q, d_k, hat_q, hat_k, d_v, o, cols, gains, acts, n_dev, n_batch, tok, head_dim):
    n_h = d_q.shape[1]
    rows, d_model = n_batch * tok, acts.shape[-1]
    width = n_h * head_dim

    def kernel(dq_ref, dk_ref, xq_ref, xk_ref, dv_ref, o_ref, c_ref, g_ref, a_ref, w_ref, b_ref, acc):
        step = pl.program_id(0)
        sides = []
        for part, (d_ref, x_ref) in enumerate(((dq_ref, xq_ref), (dk_ref, xk_ref))):
            r, c1, c2 = (c_ref[:, 3 * part + m:3 * part + m + 1] for m in range(3))
            for n in range(n_h):
                g = d_ref[:, n].reshape(rows, LANES).astype(F32) * g_ref[part * n_h + n:part * n_h + n + 1, :]
                sides.append((r * (g - c1 - x_ref[:, n].reshape(rows, LANES) * c2)).astype(BF16))
        out = lax.dot_general(jnp.concatenate(sides, axis=1), a_ref[...], (((0,), (0,)), ((), ())), preferred_element_type=F32)
        sides += [ref[:, n].reshape(rows, LANES) for ref in (dv_ref, o_ref) for n in range(n_h)]
        b_ref[0] = jnp.concatenate([a[:, :head_dim] for a in sides], axis=1)

        @pl.when(step == 0)
        def _():
            acc[...] = out

        @pl.when(step > 0)
        def _():
            acc[...] += out

        @pl.when(step == n_dev - 1)
        def _():
            for n in range(2 * n_h):
                w_ref[n * head_dim:(n + 1) * head_dim, :] = acc[n * LANES:n * LANES + head_dim, :]

    heads = pl.BlockSpec((n_batch, n_h, tok, LANES), lambda i: (0, 0, i, 0))
    return pl.pallas_call(
        kernel,
        grid=(n_dev,),
        out_shape=[jax.ShapeDtypeStruct((2 * width, d_model), F32), jax.ShapeDtypeStruct((n_dev, rows, 4 * width), BF16)],
        in_specs=[heads] * 6 + [pl.BlockSpec((rows, cols.shape[1]), lambda i: (i, 0)), pl.BlockSpec(gains.shape, lambda i: (0, 0)),
                                pl.BlockSpec((rows, d_model), lambda i: (i, 0))],
        out_specs=[pl.BlockSpec((2 * width, d_model), lambda i: (0, 0)), pl.BlockSpec((1, rows, 4 * width), lambda i: (i, 0, 0))],
        scratch_shapes=[pltpu.VMEM((2 * n_h * LANES, d_model), F32)],
        compiler_params=pltpu.CompilerParams(vmem_limit_bytes=60 * 2 ** 20),
        cost_estimate=pl.CostEstimate(flops=4 * n_dev * rows * d_model * n_h * LANES, bytes_accessed=90 * 2 ** 20, transcendentals=0),
        name='norm_back',
    )(d_q, d_k, hat_q, hat_k, d_v, o, cols, gains, acts)


def solution(mesh):
    n_dev = mesh.shape['sp']
    seq_spec = P(None, 'sp', None)
    rep_spec = P()

    def local_step(x, ln1_w, w_qkv, q_ln_w, k_ln_w, w_out, grad_y):
        n_batch, tok, d_model = x.shape
        n_heads, head_dim = q_ln_w.shape
        n_h = n_heads // n_dev
        width = n_h * head_dim
        seq = tok * n_dev
        rows = n_batch * tok
        me = lax.axis_index('sp')
        slopes = lax.dynamic_slice_in_dim(alibi_slopes(n_heads), me * n_h, n_h)

        def pad_lanes(a):
            return jnp.pad(a, ((0, 0),) * (a.ndim - 1) + ((0, LANES - head_dim),))

        x_flat = x.reshape(rows, d_model).astype(F32)
        gy = grad_y.reshape(rows, d_model)
        h_f32, ln1_pull = jax.vjp(layer_norm, x_flat, ln1_w.astype(F32))
        h_loc = h_f32.astype(BF16)
        h_all = lax.all_gather(h_loc, 'sp', axis=0, tiled=True)

        qk_raw = jnp.dot(h_loc, w_qkv[:, :2 * d_model], preferred_element_type=F32)
        stats_loc = jnp.stack(row_stats(qk_raw[:, :d_model]) + row_stats(qk_raw[:, d_model:]))
        stats = exchange(stats_loc, n_dev)
        d_o = jnp.einsum('te,nde->ntd', gy, w_out.reshape(n_dev, width, d_model), preferred_element_type=F32).astype(BF16)
        d_o = lax.all_to_all(d_o, 'sp', 0, 0, tiled=True)
        d_o = d_o.reshape(n_dev, n_batch, tok, n_h, head_dim).transpose(1, 3, 0, 2, 4).reshape(n_batch, n_h, seq, head_dim)
        d_o = pad_lanes(d_o)
        slices = [lax.dynamic_slice_in_dim(w_qkv, p * d_model + me * width, width, axis=1) for p in range(3)]
        w_pad = jnp.concatenate([pad_lanes(s[:, n * head_dim:(n + 1) * head_dim]) for s in slices for n in range(n_h)], axis=1)
        gain_q = pad_lanes(lax.dynamic_slice_in_dim(q_ln_w, me * n_h, n_h).astype(F32))
        gain_k = pad_lanes(lax.dynamic_slice_in_dim(k_ln_w, me * n_h, n_h).astype(F32))
        gains = jnp.concatenate([gain_q, gain_k])
        stats_rows = stats.transpose(0, 2, 1).reshape(n_dev * rows, 4)

        gy_late, stats_rows = lax.optimization_barrier((gy, stats_rows))
        gy_all = lax.all_gather(gy_late, 'sp', axis=0, tiled=True)
        q, k, v, hat_q, hat_k = qkv_heads(h_all, w_pad, stats_rows, gains, n_dev, n_batch, tok, seq)
        o, d_q, d_k, d_v = attention(q, k, v, d_o, slopes, head_dim, math.gcd(seq, 512))

        def gathered(a):
            return lax.all_gather(a, 'sp', axis=0, tiled=True)

        dw_v = head_grads(d_v, h_all, n_dev, n_batch, tok, head_dim)
        dw_v, d_q, d_k = lax.optimization_barrier((dw_v, d_q, d_k))
        dw_v = gathered(dw_v)

        dq32, dk32 = d_q.astype(F32), d_k.astype(F32)
        gq = dq32 * gain_q[None, :, None, :]
        gk = dk32 * gain_k[None, :, None, :]
        part = jnp.stack([jnp.sum(gq, (1, 3)), jnp.sum(gq * hat_q, (1, 3)), jnp.sum(gk, (1, 3)), jnp.sum(gk * hat_k, (1, 3))])
        part = part.reshape(4 * n_batch, n_dev, tok).transpose(1, 0, 2)
        part = exchange(part, n_dev, scatter=True)
        own = jnp.sum(part, axis=0) * (1.0 / d_model)
        full = exchange(own, n_dev).reshape(n_dev, 4, n_batch, tok).transpose(0, 2, 3, 1).reshape(n_dev * rows, 4)
        cols = jnp.concatenate([stats_rows[:, 1:2], full[:, :2], stats_rows[:, 3:4], full[:, 2:]], axis=1)
        grad_q_ln = jnp.sum(dq32 * hat_q, (0, 2))[:, :head_dim]
        grad_k_ln = jnp.sum(dk32 * hat_k, (0, 2))[:, :head_dim]

        dw_qk, back = norm_back(d_q, d_k, hat_q, hat_k, d_v, o, cols, gains, h_all, n_dev, n_batch, tok, head_dim)
        o_late, dw_qk = lax.optimization_barrier((o, dw_qk))
        dw_qk = gathered(dw_qk)
        tok_side = lax.all_to_all(back, 'sp', 0, 0, tiled=True)
        grad_w_out = gathered(head_grads(o_late, gy_all, n_dev, n_batch, tok, head_dim))
        grad_w_qkv = place_columns(None, dw_v.reshape(n_dev, 1, width, d_model), 2, 3, 4)
        grad_w_qkv = place_columns(grad_w_qkv, dw_qk.reshape(n_dev, 2, width, d_model), 0, 3, 4)

        o_tok = tok_side[:, :, 3 * width:].transpose(1, 0, 2).reshape(rows, d_model)
        y = (jnp.dot(o_tok, w_out, preferred_element_type=F32) + x_flat).astype(BF16)
        d_qkv = tok_side[:, :, :3 * width].reshape(n_dev, rows, 3, width).transpose(1, 2, 0, 3).reshape(rows, 3 * d_model)
        d_h = lax.dot_general(d_qkv, w_qkv, (((1,), (1,)), ((), ())), preferred_element_type=F32).astype(BF16)
        d_x_norm, grad_ln1 = ln1_pull(d_h.astype(F32))
        grad_x = (d_x_norm + gy.astype(F32)).astype(BF16)

        small = jnp.concatenate([grad_ln1, grad_q_ln.reshape(-1), grad_k_ln.reshape(-1)])
        n_small = small.shape[0]
        pad = -n_small % (8 * LANES)
        small_all = exchange(jnp.pad(small, (0, pad)).reshape(-1, LANES), n_dev).reshape(n_dev, n_small + pad)
        grad_ln1 = jnp.sum(small_all[:, :d_model], axis=0)
        grad_q_ln = small_all[:, d_model:d_model + width].reshape(n_heads, head_dim)
        grad_k_ln = small_all[:, d_model + width:d_model + 2 * width].reshape(n_heads, head_dim)
        shape = (n_batch, tok, d_model)
        return y.reshape(shape), grad_x.reshape(shape), grad_ln1, grad_w_qkv, grad_q_ln, grad_k_ln, grad_w_out

    return jax.shard_map(local_step, mesh=mesh, in_specs=(seq_spec, rep_spec, rep_spec, rep_spec, rep_spec, rep_spec, seq_spec), out_specs=(seq_spec, seq_spec, rep_spec, rep_spec, rep_spec, rep_spec, rep_spec), check_vma=False)
```

```python
import math
import jax
import jax.numpy as jnp
from jax import lax
from jax.experimental import pallas as pl
from jax.experimental.pallas import tpu as pltpu
from jax.sharding import PartitionSpec as P

F32 = jnp.float32
BF16 = jnp.bfloat16
LANES = 128
LOG2E = math.log2(math.e)
MESH = pl.DeviceIdType.MESH


def alibi_slopes(n_heads):
    pow_two = 2 ** math.ceil(math.log2(n_heads))
    exponents = jnp.arange(1, pow_two + 1, dtype=F32) * (8.0 / pow_two)
    slopes = jnp.exp2(-exponents)
    if pow_two != n_heads:
        slopes = jnp.concatenate([slopes[1::2], slopes[0::2]])[:n_heads]
    return slopes


def layer_norm(values, weight):
    centered = values - jnp.mean(values, axis=-1, keepdims=True)
    var_val = jnp.mean(centered * centered, axis=-1, keepdims=True)
    return centered * lax.rsqrt(var_val + 1e-5) * weight


def row_stats(values):
    mean = jnp.mean(values, axis=-1, keepdims=True)
    centered = values - mean
    var_val = jnp.mean(centered * centered, axis=-1)
    return mean[..., 0], lax.rsqrt(var_val + 1e-5)


def exchange(block, n_dev, scatter=False):
    shape = block.shape[1:] if scatter else block.shape

    def kernel(x_ref, o_ref, loc_sem, send_sem, recv_sem):
        me = lax.axis_index('sp')
        src = (lambda dev: x_ref.at[dev]) if scatter else (lambda dev: x_ref)
        own = pltpu.make_async_copy(src(me), o_ref.at[me], loc_sem)
        own.start()
        copies = []
        for step in range(1, n_dev):
            peer = lax.rem(me + step, n_dev)
            copies.append(pltpu.make_async_remote_copy(
                src_ref=src(peer), dst_ref=o_ref.at[me], send_sem=send_sem.at[step], recv_sem=recv_sem.at[step],
                device_id=(peer,), device_id_type=MESH))
            copies[-1].start()
        own.wait()
        for copy in copies:
            copy.wait()

    return pl.pallas_call(
        kernel,
        out_shape=jax.ShapeDtypeStruct((n_dev,) + shape, block.dtype),
        in_specs=[pl.BlockSpec(memory_space=pl.ANY)],
        out_specs=pl.BlockSpec(memory_space=pl.ANY),
        scratch_shapes=[pltpu.SemaphoreType.DMA, pltpu.SemaphoreType.DMA((n_dev,)), pltpu.SemaphoreType.DMA((n_dev,))],
        compiler_params=pltpu.CompilerParams(has_side_effects=True),
        name='scatter_rows' if scatter else 'exchange',
    )(block)


def norm_rows(x, weight, blk):
    rows, d_model = x.shape

    def kernel(x_ref, w_ref, o_ref):
        o_ref[...] = layer_norm(x_ref[...].astype(F32), w_ref[...]).astype(BF16)

    return pl.pallas_call(
        kernel,
        grid=(rows // blk,),
        out_shape=jax.ShapeDtypeStruct(x.shape, BF16),
        in_specs=[pl.BlockSpec((blk, d_model), lambda i: (i, 0)), pl.BlockSpec((1, d_model), lambda i: (0, 0))],
        out_specs=pl.BlockSpec((blk, d_model), lambda i: (i, 0)),
        cost_estimate=pl.CostEstimate(flops=8 * rows * d_model, bytes_accessed=4 * rows * d_model, transcendentals=0),
        name='norm_rows',
    )(x, weight)


def columns_of(weight, rows_in, blk):
    n_out, d_in = weight.shape
    rows = rows_in.shape[0]

    def kernel(w_ref, r_ref, o_ref):
        o_ref[...] = lax.dot_general(w_ref[...], r_ref[...], (((1,), (1,)), ((), ())), preferred_element_type=F32).astype(BF16)

    return pl.pallas_call(
        kernel,
        grid=(n_out // blk,),
        out_shape=jax.ShapeDtypeStruct((n_out, rows), BF16),
        in_specs=[pl.BlockSpec((blk, d_in), lambda i: (i, 0)), pl.BlockSpec((rows, d_in), lambda i: (0, 0))],
        out_specs=pl.BlockSpec((blk, rows), lambda i: (i, 0)),
        compiler_params=pltpu.CompilerParams(vmem_limit_bytes=40 * 2 ** 20),
        cost_estimate=pl.CostEstimate(flops=2 * n_out * d_in * rows, bytes_accessed=2 * (n_out + rows) * d_in, transcendentals=0),
        name='columns_of',
    )(weight, rows_in)


def token_cols(block, n_batch):
    return jnp.concatenate([block[8 * b:8 * b + 8, :].T for b in range(n_batch)], axis=0)


def qkv_heads(h_all, w_pad, stats, gains, n_dev, n_batch, tok, seq):
    rows = n_batch * tok
    d_model = h_all.shape[-1]
    n_h = gains.shape[0] // 2

    def kernel(h_ref, w_ref, st_ref, g_ref, q_ref, k_ref, v_ref, xq_ref, xk_ref):
        raw = jnp.dot(h_ref[...], w_ref[...], preferred_element_type=F32)
        st = token_cols(st_ref[0], n_batch)
        for n in range(n_h):
            for part, (o_ref, x_ref) in enumerate(((q_ref, xq_ref), (k_ref, xk_ref))):
                col = (part * n_h + n) * LANES
                hat = (raw[:, col:col + LANES] - st[:, 2 * part:2 * part + 1]) * st[:, 2 * part + 1:2 * part + 2]
                out = (hat * g_ref[part * n_h + n:part * n_h + n + 1, :]).astype(BF16)
                x_ref[:, n] = hat.reshape(n_batch, tok, LANES)
                o_ref[:, n] = out.reshape(n_batch, tok, LANES)
            col = (2 * n_h + n) * LANES
            v_ref[:, n] = raw[:, col:col + LANES].astype(BF16).reshape(n_batch, tok, LANES)

    shape = (n_batch, n_h, seq, LANES)
    spec = pl.BlockSpec((n_batch, n_h, tok, LANES), lambda i: (0, 0, i, 0))
    n_col = w_pad.shape[1]
    return pl.pallas_call(
        kernel,
        grid=(n_dev,),
        out_shape=[jax.ShapeDtypeStruct(shape, BF16)] * 3 + [jax.ShapeDtypeStruct(shape, F32)] * 2,
        in_specs=[pl.BlockSpec((rows, d_model), lambda i: (i, 0)), pl.BlockSpec((d_model, n_col), lambda i: (0, 0)),
                  pl.BlockSpec((1,) + stats.shape[1:], lambda i: (i, 0, 0)), pl.BlockSpec(gains.shape, lambda i: (0, 0))],
        out_specs=[spec] * 5,
        compiler_params=pltpu.CompilerParams(vmem_limit_bytes=60 * 2 ** 20),
        cost_estimate=pl.CostEstimate(flops=2 * n_dev * rows * d_model * n_col, bytes_accessed=80 * 2 ** 20, transcendentals=0),
        name='qkv_heads',
    )(h_all, w_pad, stats, gains)


def attention(q, k, v, d_o, hat_q, hat_k, gains, slopes, head_dim, blk):
    n_batch, n_h, seq, _ = q.shape
    n_blk = seq // blk
    tok = d_o.shape[-1] // n_batch
    n_grp = blk // tok
    scale = head_dim ** -0.5

    def dot(a, b):
        return jnp.dot(a, b, preferred_element_type=F32)

    def kernel(slope_ref, q_ref, k_ref, v_ref, do_ref, xq_ref, xk_ref, gq_ref, gk_ref, o_ref, dq_ref, dk_ref, dv_ref, sum_ref, gl_ref, w_ref, dk_acc, dv_acc, kt_ref, vt_ref):
        slope2 = slope_ref[pl.program_id(1)] * LOG2E
        dk_acc[...] = jnp.zeros_like(dk_acc)
        dv_acc[...] = jnp.zeros_like(dv_acc)
        kt_ref[...] = k_ref[0, 0].T
        vt_ref[...] = v_ref[0, 0].T
        sum_ref[...] = jnp.zeros_like(sum_ref)
        gl_ref[...] = jnp.zeros_like(gl_ref)

        def norm_terms(part, rows, d_b, x_ref, g_ref):
            gain = g_ref[0]
            prod = d_b.astype(F32) * x_ref[0, 0, rows, :]
            gl_ref[0, 0, part:part + 1, :] += jnp.sum(prod, axis=0, keepdims=True)
            prod = prod * gain
            pieces = [d_b]
            for _ in range(3):
                pieces.append(prod.astype(BF16))
                prod = prod - pieces[-1].astype(F32)
            row = lax.broadcasted_iota(jnp.int32, (8, LANES), 0)
            first = jnp.where(row == 0, jnp.broadcast_to(gain, (8, LANES)), 0.0).astype(BF16)
            other = jnp.where(row == 1, 1.0, 0.0).astype(BF16)
            lhs = jnp.concatenate([first, other, other, other], axis=1)
            both = lax.dot_general(lhs, jnp.concatenate(pieces, axis=1), (((1,), (1,)), ((), ())), preferred_element_type=F32)
            sum_ref[0, 0, 2 * part:2 * part + 2, rows] = both[:2]

        key_iota = lax.broadcasted_iota(jnp.int32, (blk, LANES), 0)[:, :1]
        blocks = [pl.ds(j * blk, blk) for j in range(n_blk)]

        for i in range(n_blk):
            q_b = q_ref[0, 0, blocks[i], :]
            q_t = q_b.T
            do_t = jnp.concatenate([do_ref[i * n_grp + m, 0] for m in range(n_grp)], axis=1)
            do_t = jnp.concatenate([do_t, jnp.zeros((LANES - head_dim, blk), BF16)], axis=0)
            do_b = do_t.T
            top = None
            for j in range(i, -1, -1):
                s = dot(k_ref[0, 0, blocks[j], :], q_t) * (scale * LOG2E)
                s = s + (key_iota + (j - i) * blk).astype(F32) * slope2
                if i == j:
                    key_pos = lax.broadcasted_iota(jnp.int32, (blk, blk), 0)
                    q_pos = lax.broadcasted_iota(jnp.int32, (blk, blk), 1)
                    s = jnp.where(key_pos <= q_pos, s, -1e30)
                w_ref[blocks[j], :] = s
                peak = jnp.max(s, axis=0, keepdims=True)
                top = peak if top is None else jnp.maximum(top, peak)

            total = jnp.zeros((1, blk), F32)
            out_t = jnp.zeros((LANES, blk), F32)
            for j in range(i + 1):
                w = jnp.exp2(w_ref[blocks[j], :] - top)
                w_ref[blocks[j], :] = w
                out_t = out_t + dot(vt_ref[:, blocks[j]], w.astype(BF16))
                total = total + jnp.sum(w, axis=0, keepdims=True)
            inv = 1.0 / total
            out_b = (out_t * inv).T.astype(BF16)
            o_ref[0, 0, blocks[i], :] = out_b
            delta = jnp.sum((out_b.astype(F32) * do_b.astype(F32)).T, axis=0, keepdims=True)

            dq_t = jnp.zeros((LANES, blk), F32)
            for j in range(i + 1):
                d_p = dot(v_ref[0, 0, blocks[j], :], do_t)
                p = w_ref[blocks[j], :] * inv
                dv_acc[blocks[j], :] += dot(p.astype(BF16), do_b)
                d_s = (p * (d_p - delta)).astype(BF16)
                dk_acc[blocks[j], :] += dot(d_s, q_b)
                dq_t = dq_t + dot(kt_ref[:, blocks[j]], d_s)
            dq_b = (dq_t * scale).T.astype(BF16)
            dq_ref[0, 0, blocks[i], :] = dq_b
            norm_terms(0, blocks[i], dq_b, xq_ref, gq_ref)

        for j in range(n_blk):
            dk_b = (dk_acc[blocks[j], :] * scale).astype(BF16)
            dk_ref[0, 0, blocks[j], :] = dk_b
            norm_terms(1, blocks[j], dk_b, xk_ref, gk_ref)
        dv_ref[0, 0] = dv_acc[...].astype(BF16)

    spec = pl.BlockSpec((1, 1, seq, LANES), lambda b, n: (b, n, 0, 0))
    flops = 6 * 2 * n_batch * n_h * seq * seq * LANES
    return pl.pallas_call(
        kernel,
        grid=(n_batch, n_h),
        out_shape=[jax.ShapeDtypeStruct(q.shape, BF16)] * 4 + [jax.ShapeDtypeStruct((n_batch, n_h, 8, n), F32) for n in (seq, LANES)],
        in_specs=[pl.BlockSpec(memory_space=pltpu.SMEM)] + [spec] * 3 + [pl.BlockSpec((seq // tok, 1, head_dim, tok), lambda b, n: (0, n, 0, b))] + [spec] * 2 + [pl.BlockSpec((1, 1, LANES), lambda b, n: (n, 0, 0)), pl.BlockSpec((1, 1, LANES), lambda b, n: (n_h + n, 0, 0))],
        out_specs=[spec] * 4 + [pl.BlockSpec((1, 1, 8, n), lambda b, n: (b, n, 0, 0)) for n in (seq, LANES)],
        scratch_shapes=[pltpu.VMEM((seq, blk), F32), pltpu.VMEM((seq, LANES), F32), pltpu.VMEM((seq, LANES), F32),
                        pltpu.VMEM((LANES, seq), BF16), pltpu.VMEM((LANES, seq), BF16)],
        compiler_params=pltpu.CompilerParams(vmem_limit_bytes=60 * 2 ** 20),
        cost_estimate=pl.CostEstimate(flops=flops, bytes_accessed=40 * 2 ** 20, transcendentals=n_batch * n_h * seq * seq // 2),
        name='attention',
    )(slopes, q, k, v, d_o, hat_q, hat_k, gains[:, None], gains[:, None])


def place_columns(buf, gathered, first, n_part, group, parts=1):
    n_dev, _, d_in = gathered.shape
    width = d_in // n_dev
    mb = 512 if d_in % 512 == 0 else d_in
    n_grp = n_dev // group

    def kernel(x_ref, *refs):
        refs[-1][...] = x_ref[...].reshape(group * width, mb).T

    args = (gathered,) if buf is None else (gathered, buf)
    return pl.pallas_call(
        kernel,
        grid=(parts, n_grp, d_in // mb),
        out_shape=jax.ShapeDtypeStruct((d_in, n_part * n_dev * width), gathered.dtype),
        in_specs=[pl.BlockSpec((group, width, mb), lambda p, g, m: (g, p, m))] + [pl.BlockSpec(memory_space=pl.ANY)] * (len(args) - 1),
        out_specs=pl.BlockSpec((mb, group * width), lambda p, g, m: (m, (p + first) * n_grp + g)),
        input_output_aliases={1: 0} if buf is not None else {},
        compiler_params=pltpu.CompilerParams(vmem_limit_bytes=40 * 2 ** 20),
        cost_estimate=pl.CostEstimate(flops=parts * d_in * d_in, bytes_accessed=8 * parts * d_in * d_in, transcendentals=0),
        name='place_columns',
    )(*args)


def place_rows(buf, gathered, first, n_rows, half, n_half):
    n_dev, _, d_in = gathered.shape
    group = math.gcd(n_dev, 4)

    def kernel(x_ref, *refs):
        refs[-1][:, 0] = x_ref[...]

    args = (gathered,) if buf is None else (gathered, buf)
    return pl.pallas_call(
        kernel,
        grid=(n_dev // group,),
        out_shape=jax.ShapeDtypeStruct((n_dev, n_half, n_rows, d_in), gathered.dtype),
        in_specs=[pl.BlockSpec((group, n_rows, d_in), lambda i: (i, first // n_rows, 0))] + [pl.BlockSpec(memory_space=pl.ANY)] * (len(args) - 1),
        out_specs=pl.BlockSpec((group, 1, n_rows, d_in), lambda i: (i, half, 0, 0)),
        input_output_aliases={1: 0} if buf is not None else {},
        compiler_params=pltpu.CompilerParams(vmem_limit_bytes=40 * 2 ** 20),
        cost_estimate=pl.CostEstimate(flops=n_dev * n_rows * d_in, bytes_accessed=8 * n_dev * n_rows * d_in, transcendentals=0),
        name='place_rows',
    )(*args)


def token_rows(arrays, n_dev, n_batch, tok, head_dim):
    n_h = arrays[0].shape[1]
    rows = n_batch * tok
    width = len(arrays) * n_h * head_dim

    def kernel(*refs):
        refs[-1][0] = jnp.concatenate([ref[:, n].reshape(rows, LANES).T[:head_dim] for ref in refs[:-1] for n in range(n_h)], axis=0)

    return pl.pallas_call(
        kernel,
        grid=(n_dev,),
        out_shape=jax.ShapeDtypeStruct((n_dev, width, rows), BF16),
        in_specs=[pl.BlockSpec((n_batch, n_h, tok, LANES), lambda i: (0, 0, i, 0))] * len(arrays),
        out_specs=pl.BlockSpec((1, width, rows), lambda i: (i, 0, 0)),
        cost_estimate=pl.CostEstimate(flops=n_dev * rows * width, bytes_accessed=4 * n_dev * rows * width, transcendentals=0),
        name='token_rows',
    )(*arrays)


def head_grads(side, acts, n_dev, n_batch, tok, head_dim):
    n_h = side.shape[1]
    rows, d_model = n_batch * tok, acts.shape[-1]

    def kernel(s_ref, a_ref, o_ref, acc):
        step = pl.program_id(0)
        lhs = jnp.concatenate([s_ref[:, n].reshape(rows, LANES) for n in range(n_h)], axis=1)

        @pl.when(step == 0)
        def _():
            acc[...] = jnp.zeros_like(acc)

        acc[...] += lax.dot_general(lhs, a_ref[...], (((0,), (0,)), ((), ())), preferred_element_type=F32)

        @pl.when(step == n_dev - 1)
        def _():
            for n in range(n_h):
                o_ref[n * head_dim:(n + 1) * head_dim, :] = acc[n * LANES:n * LANES + head_dim, :]

    return pl.pallas_call(
        kernel,
        grid=(n_dev,),
        out_shape=jax.ShapeDtypeStruct((n_h * head_dim, d_model), F32),
        in_specs=[pl.BlockSpec((n_batch, n_h, tok, LANES), lambda i: (0, 0, i, 0)), pl.BlockSpec((rows, d_model), lambda i: (i, 0))],
        out_specs=pl.BlockSpec((n_h * head_dim, d_model), lambda i: (0, 0)),
        scratch_shapes=[pltpu.VMEM((n_h * LANES, d_model), F32)],
        compiler_params=pltpu.CompilerParams(vmem_limit_bytes=50 * 2 ** 20),
        cost_estimate=pl.CostEstimate(flops=2 * n_dev * rows * d_model * n_h * LANES, bytes_accessed=50 * 2 ** 20, transcendentals=0),
        name='head_grads',
    )(side, acts)


def norm_back(d_q, d_k, hat_q, hat_k, stats, sums, gains, acts, n_dev, n_batch, tok, head_dim):
    n_h = d_q.shape[1]
    rows, d_model = n_batch * tok, acts.shape[-1]
    width = n_h * head_dim

    def kernel(dq_ref, dk_ref, xq_ref, xk_ref, st_ref, c_ref, g_ref, a_ref, w_ref, b_ref, acc):
        step = pl.program_id(0)
        st = token_cols(st_ref[0], n_batch)
        cols = token_cols(c_ref[0], n_batch)
        sides = []
        for part, (d_ref, x_ref) in enumerate(((dq_ref, xq_ref), (dk_ref, xk_ref))):
            r = st[:, 2 * part + 1:2 * part + 2]
            c1, c2 = (cols[:, 2 * part + m:2 * part + m + 1] for m in range(2))
            for n in range(n_h):
                g = d_ref[:, n].reshape(rows, LANES).astype(F32) * g_ref[part * n_h + n:part * n_h + n + 1, :]
                sides.append((r * (g - c1 - x_ref[:, n].reshape(rows, LANES) * c2)).astype(BF16))
        b_ref[0] = jnp.concatenate([a.T[:head_dim] for a in sides], axis=0)

        @pl.when(step == 0)
        def _():
            acc[...] = jnp.zeros_like(acc)

        acc[...] += lax.dot_general(jnp.concatenate(sides, axis=1), a_ref[...], (((0,), (0,)), ((), ())), preferred_element_type=F32)

        @pl.when(step == n_dev - 1)
        def _():
            for n in range(2 * n_h):
                w_ref[n * head_dim:(n + 1) * head_dim, :] = acc[n * LANES:n * LANES + head_dim, :]

    heads = pl.BlockSpec((n_batch, n_h, tok, LANES), lambda i: (0, 0, i, 0))
    return pl.pallas_call(
        kernel,
        grid=(n_dev,),
        out_shape=[jax.ShapeDtypeStruct((2 * width, d_model), F32), jax.ShapeDtypeStruct((n_dev, 2 * width, rows), BF16)],
        in_specs=[heads] * 4 + [pl.BlockSpec((1,) + stats.shape[1:], lambda i: (i, 0, 0))] * 2 + [pl.BlockSpec(gains.shape, lambda i: (0, 0)),
                                pl.BlockSpec((rows, d_model), lambda i: (i, 0))],
        out_specs=[pl.BlockSpec((2 * width, d_model), lambda i: (0, 0)), pl.BlockSpec((1, 2 * width, rows), lambda i: (i, 0, 0))],
        scratch_shapes=[pltpu.VMEM((2 * n_h * LANES, d_model), F32)],
        compiler_params=pltpu.CompilerParams(vmem_limit_bytes=60 * 2 ** 20),
        cost_estimate=pl.CostEstimate(flops=4 * n_dev * rows * d_model * n_h * LANES, bytes_accessed=90 * 2 ** 20, transcendentals=0),
        name='norm_back',
    )(d_q, d_k, hat_q, hat_k, stats, sums, gains, acts)


def solution(mesh):
    n_dev = mesh.shape['sp']
    seq_spec = P(None, 'sp', None)
    rep_spec = P()

    def local_step(x, ln1_w, w_qkv, q_ln_w, k_ln_w, w_out, grad_y):
        n_batch, tok, d_model = x.shape
        n_heads, head_dim = q_ln_w.shape
        n_h = n_heads // n_dev
        width = n_h * head_dim
        seq = tok * n_dev
        rows = n_batch * tok
        me = lax.axis_index('sp')
        slopes = lax.dynamic_slice_in_dim(alibi_slopes(n_heads), me * n_h, n_h)

        def pad_lanes(a):
            return jnp.pad(a, ((0, 0),) * (a.ndim - 1) + ((0, LANES - head_dim),))

        x_flat = x.reshape(rows, d_model).astype(F32)
        gy = grad_y.reshape(rows, d_model)
        h_loc = norm_rows(x.reshape(rows, d_model), ln1_w.astype(F32).reshape(1, d_model), math.gcd(rows, 128))
        h_all = lax.all_gather(h_loc, 'sp', axis=0, tiled=True)

        qk_raw = jnp.dot(h_loc, w_qkv[:, :2 * d_model], preferred_element_type=F32)
        stats_loc = jnp.stack(row_stats(qk_raw[:, :d_model]) + row_stats(qk_raw[:, d_model:])).reshape(4, n_batch, tok)
        stats_loc = jnp.pad(stats_loc.transpose(1, 0, 2), ((0, 0), (0, 4), (0, 0))).reshape(8 * n_batch, tok)
        stats = exchange(stats_loc, n_dev)
        d_o = columns_of(w_out, gy, 4 * width).reshape(n_dev, width, rows)
        d_o, h_all = lax.optimization_barrier((d_o, h_all))
        d_o = lax.all_to_all(d_o, 'sp', 0, 0, tiled=True)
        d_o = d_o.reshape(n_dev, n_h, head_dim, rows)
        slices = [lax.dynamic_slice_in_dim(w_qkv, p * d_model + me * width, width, axis=1) for p in range(3)]
        w_pad = jnp.concatenate([pad_lanes(s[:, n * head_dim:(n + 1) * head_dim]) for s in slices for n in range(n_h)], axis=1)
        gain_q = pad_lanes(lax.dynamic_slice_in_dim(q_ln_w, me * n_h, n_h).astype(F32))
        gain_k = pad_lanes(lax.dynamic_slice_in_dim(k_ln_w, me * n_h, n_h).astype(F32))
        gains = jnp.concatenate([gain_q, gain_k])

        gy_late, stats = lax.optimization_barrier((gy, stats))
        gy_all = lax.all_gather(gy_late, 'sp', axis=0, tiled=True)
        q, k, v, hat_q, hat_k = qkv_heads(h_all, w_pad, stats, gains, n_dev, n_batch, tok, seq)
        o, d_q, d_k, d_v, head_sums, head_ln = attention(q, k, v, d_o, hat_q, hat_k, gains, slopes, head_dim, math.gcd(seq, 512))

        def gathered(a):
            return lax.all_gather(a, 'sp', axis=0, tiled=True)

        dw_v = head_grads(d_v, h_all, n_dev, n_batch, tok, head_dim)
        dw_v, d_q, d_k, head_sums = lax.optimization_barrier((dw_v, d_q, d_k, head_sums))
        dw_v = gathered(dw_v)

        part = jnp.sum(head_sums, axis=1).reshape(n_batch, 8, n_dev, tok).transpose(2, 0, 1, 3).reshape(n_dev, 8 * n_batch, tok)
        grad_q_ln, grad_k_ln = jnp.sum(head_ln, axis=0)[:, :2, :head_dim].transpose(1, 0, 2)
        part = exchange(part, n_dev, scatter=True)
        sums = exchange(jnp.sum(part, axis=0) * (1.0 / d_model), n_dev)

        d_v, o, sums = lax.optimization_barrier((d_v, o, sums))
        tok_ov = lax.all_to_all(token_rows((d_v, o), n_dev, n_batch, tok, head_dim), 'sp', 0, 0, tiled=True)
        dw_qk, back_qk = norm_back(d_q, d_k, hat_q, hat_k, stats, sums, gains, h_all, n_dev, n_batch, tok, head_dim)
        tok_qk = lax.all_to_all(back_qk, 'sp', 0, 0, tiled=True)
        o_late, dw_qk = lax.optimization_barrier((o, dw_qk))
        dw_out = head_grads(o_late, gy_all, n_dev, n_batch, tok, head_dim)
        half = width // 2
        dw_qko = gathered(jnp.concatenate([dw_qk, dw_out[:half]])).reshape(n_dev, 2 * width + half, d_model)
        dw_last = gathered(dw_out[half:]).reshape(n_dev, half, d_model)
        grad_w_qkv = place_columns(None, dw_v.reshape(n_dev, width, d_model), 2, 3, 4)
        grad_w_qkv = place_columns(grad_w_qkv, dw_qko, 0, 3, 4, parts=2)
        grad_w_out = place_rows(None, dw_qko, 2 * width, half, 0, 2)
        grad_w_out = place_rows(grad_w_out, dw_last, 0, half, 1, 2).reshape(d_model, d_model)

        def over_rows(cols, weight, w_dim):
            return lax.dot_general(cols, weight, (((0,), (w_dim,)), ((), ())), preferred_element_type=F32)

        o_cols = tok_ov[:, width:].reshape(d_model, rows)
        y = (over_rows(o_cols, w_out, 0) + x_flat).astype(BF16)
        d_cols = jnp.stack([tok_qk[:, :width], tok_qk[:, width:], tok_ov[:, :width]]).reshape(3 * d_model, rows)
        d_h = over_rows(d_cols, w_qkv, 1).astype(BF16)
        _, ln1_pull = jax.vjp(layer_norm, x_flat, ln1_w.astype(F32))
        d_x_norm, grad_ln1 = ln1_pull(d_h.astype(F32))
        grad_x = (d_x_norm + gy.astype(F32)).astype(BF16)

        small = jnp.concatenate([grad_ln1, grad_q_ln.reshape(-1), grad_k_ln.reshape(-1)])
        n_small = small.shape[0]
        pad = -n_small % (8 * LANES)
        small_all = exchange(jnp.pad(small, (0, pad)).reshape(-1, LANES), n_dev).reshape(n_dev, n_small + pad)
        grad_ln1 = jnp.sum(small_all[:, :d_model], axis=0)
        grad_q_ln = small_all[:, d_model:d_model + width].reshape(n_heads, head_dim)
        grad_k_ln = small_all[:, d_model + width:d_model + 2 * width].reshape(n_heads, head_dim)
        shape = (n_batch, tok, d_model)
        return y.reshape(shape), grad_x.reshape(shape), grad_ln1, grad_w_qkv, grad_q_ln, grad_k_ln, grad_w_out

    return jax.shard_map(local_step, mesh=mesh, in_specs=(seq_spec, rep_spec, rep_spec, rep_spec, rep_spec, rep_spec, seq_spec), out_specs=(seq_spec, seq_spec, rep_spec, rep_spec, rep_spec, rep_spec, rep_spec), check_vma=False)
```

```python
import math
import jax
import jax.numpy as jnp
from jax import lax
from jax.experimental import pallas as pl
from jax.experimental.pallas import tpu as pltpu
from jax.sharding import PartitionSpec as P

F32 = jnp.float32
BF16 = jnp.bfloat16
LANES = 128
LOG2E = math.log2(math.e)
MESH = pl.DeviceIdType.MESH


def alibi_slopes(n_heads):
    pow_two = 2 ** math.ceil(math.log2(n_heads))
    exponents = jnp.arange(1, pow_two + 1, dtype=F32) * (8.0 / pow_two)
    slopes = jnp.exp2(-exponents)
    if pow_two != n_heads:
        slopes = jnp.concatenate([slopes[1::2], slopes[0::2]])[:n_heads]
    return slopes


def layer_norm(values, weight):
    centered = values - jnp.mean(values, axis=-1, keepdims=True)
    var_val = jnp.mean(centered * centered, axis=-1, keepdims=True)
    return centered * lax.rsqrt(var_val + 1e-5) * weight


def exchange(block, n_dev, scatter=False):
    shape = block.shape[1:] if scatter else block.shape

    def kernel(x_ref, o_ref, loc_sem, send_sem, recv_sem):
        me = lax.axis_index('sp')
        src = (lambda dev: x_ref.at[dev]) if scatter else (lambda dev: x_ref)
        own = pltpu.make_async_copy(src(me), o_ref.at[me], loc_sem)
        own.start()

        def copy(step):
            peer = lax.rem(me + step, n_dev)
            return pltpu.make_async_remote_copy(
                src_ref=src(peer), dst_ref=o_ref.at[me], send_sem=send_sem.at[step], recv_sem=recv_sem.at[step],
                device_id=(peer,), device_id_type=MESH)

        @pl.loop(1, n_dev)
        def _(step):
            copy(step).start()

        own.wait()

        @pl.loop(1, n_dev)
        def _(step):
            copy(step).wait()

    return pl.pallas_call(
        kernel,
        out_shape=jax.ShapeDtypeStruct((n_dev,) + shape, block.dtype),
        in_specs=[pl.BlockSpec(memory_space=pl.ANY)],
        out_specs=pl.BlockSpec(memory_space=pl.ANY),
        scratch_shapes=[pltpu.SemaphoreType.DMA, pltpu.SemaphoreType.DMA((n_dev,)), pltpu.SemaphoreType.DMA((n_dev,))],
        compiler_params=pltpu.CompilerParams(has_side_effects=True),
        name='scatter_rows' if scatter else 'exchange',
    )(block)


def norm_rows(x, weight, blk):
    rows, d_model = x.shape

    def kernel(x_ref, w_ref, o_ref):
        o_ref[...] = layer_norm(x_ref[...].astype(F32), w_ref[...]).astype(BF16)

    return pl.pallas_call(
        kernel,
        grid=(rows // blk,),
        out_shape=jax.ShapeDtypeStruct(x.shape, BF16),
        in_specs=[pl.BlockSpec((blk, d_model), lambda i: (i, 0)), pl.BlockSpec((1, d_model), lambda i: (0, 0))],
        out_specs=pl.BlockSpec((blk, d_model), lambda i: (i, 0)),
        cost_estimate=pl.CostEstimate(flops=8 * rows * d_model, bytes_accessed=4 * rows * d_model, transcendentals=0),
        name='norm_rows',
    )(x, weight)


def columns_of(weight, rows_in, blk):
    n_out, d_in = weight.shape
    rows = rows_in.shape[0]

    def kernel(w_ref, r_ref, o_ref):
        o_ref[...] = lax.dot_general(w_ref[...], r_ref[...], (((1,), (1,)), ((), ())), preferred_element_type=F32).astype(BF16)

    return pl.pallas_call(
        kernel,
        grid=(n_out // blk,),
        out_shape=jax.ShapeDtypeStruct((n_out, rows), BF16),
        in_specs=[pl.BlockSpec((blk, d_in), lambda i: (i, 0)), pl.BlockSpec((rows, d_in), lambda i: (0, 0))],
        out_specs=pl.BlockSpec((blk, rows), lambda i: (i, 0)),
        compiler_params=pltpu.CompilerParams(vmem_limit_bytes=40 * 2 ** 20),
        cost_estimate=pl.CostEstimate(flops=2 * n_out * d_in * rows, bytes_accessed=2 * (n_out + rows) * d_in, transcendentals=0),
        name='columns_of',
    )(weight, rows_in)


def column_stats(h, w_qkv, blk):
    rows, d_model = h.shape
    n_blk = d_model // blk

    def kernel(h_ref, w_ref, o_ref, raw):
        c = pl.program_id(1)
        raw[c] = jnp.dot(h_ref[...], w_ref[...], preferred_element_type=F32)

        @pl.when(c == n_blk - 1)
        def _():
            mean = sum(jnp.sum(raw[m], axis=1, keepdims=True) for m in range(n_blk)) * (1.0 / d_model)
            sq = jnp.zeros((rows, 1), F32)
            for m in range(n_blk):
                centered = raw[m] - mean
                sq = sq + jnp.sum(centered * centered, axis=1, keepdims=True)
            rstd = lax.rsqrt(sq * (1.0 / d_model) + 1e-5)
            lane = lax.broadcasted_iota(jnp.int32, (rows, LANES), 1)
            o_ref[0] = jnp.where(lane == 0, mean, rstd)

    return pl.pallas_call(
        kernel,
        grid=(2, n_blk),
        out_shape=jax.ShapeDtypeStruct((2, rows, LANES), F32),
        in_specs=[pl.BlockSpec((rows, d_model), lambda p, c: (0, 0)), pl.BlockSpec((d_model, blk), lambda p, c: (0, p * n_blk + c))],
        out_specs=pl.BlockSpec((1, rows, LANES), lambda p, c: (p, 0, 0)),
        scratch_shapes=[pltpu.VMEM((n_blk, rows, blk), F32)],
        compiler_params=pltpu.CompilerParams(vmem_limit_bytes=50 * 2 ** 20),
        cost_estimate=pl.CostEstimate(flops=4 * rows * d_model * d_model, bytes_accessed=4 * d_model * d_model, transcendentals=0),
        name='column_stats',
    )(h, w_qkv)


def project_out(tok_ov, w_out, x, group):
    rows, d_model = x.shape
    n_dev, width = tok_ov.shape[0], tok_ov.shape[1] // 2
    steps = n_dev // group

    def kernel(o_ref, w_ref, x_ref, y_ref, acc):
        step = pl.program_id(0)

        @pl.when(step == 0)
        def _():
            acc[...] = x_ref[...].astype(F32)

        acc[...] += lax.dot_general(o_ref[...].reshape(group * width, rows), w_ref[...], (((0,), (0,)), ((), ())), preferred_element_type=F32)

        @pl.when(step == steps - 1)
        def _():
            y_ref[...] = acc[...].astype(BF16)

    return pl.pallas_call(
        kernel,
        grid=(steps,),
        out_shape=jax.ShapeDtypeStruct((rows, d_model), BF16),
        in_specs=[pl.BlockSpec((group, width, rows), lambda i: (i, 1, 0)), pl.BlockSpec((group * width, d_model), lambda i: (i, 0)),
                  pl.BlockSpec((rows, d_model), lambda i: (0, 0))],
        out_specs=pl.BlockSpec((rows, d_model), lambda i: (0, 0)),
        scratch_shapes=[pltpu.VMEM((rows, d_model), F32)],
        compiler_params=pltpu.CompilerParams(vmem_limit_bytes=50 * 2 ** 20),
        cost_estimate=pl.CostEstimate(flops=2 * rows * d_model * d_model, bytes_accessed=2 * d_model * d_model, transcendentals=0),
        name='project_out',
    )(tok_ov, w_out, x)


def token_grads(tok_qk, tok_ov, w_qkv, x, ln_w, gy, group, chunk):
    rows, d_model = x.shape
    n_dev, width = tok_ov.shape[0], tok_ov.shape[1] // 2
    steps = n_dev // group

    def kernel(qk_ref, v_ref, w_ref, x_ref, l_ref, y_ref, o_ref, gl_ref, acc):
        part, step = pl.program_id(0), pl.program_id(1)

        @pl.when((part == 0) & (step == 0))
        def _():
            acc[...] = jnp.zeros_like(acc)

        side = jnp.where(part == 2, v_ref[...], qk_ref[...]).reshape(group * width, rows)
        acc[...] += lax.dot_general(side, w_ref[...], (((0,), (1,)), ((), ())), preferred_element_type=F32)

        @pl.when((part == 2) & (step == steps - 1))
        def _():
            gl_ref[...] = jnp.zeros_like(gl_ref)

            @pl.loop(0, rows // chunk)
            def _(m):
                at = pl.ds(pl.multiple_of(m * chunk, chunk), chunk)
                xs = x_ref[at, :].astype(F32)
                centered = xs - jnp.mean(xs, axis=1, keepdims=True)
                rstd = lax.rsqrt(jnp.mean(centered * centered, axis=1, keepdims=True) + 1e-5)
                hat = centered * rstd
                d_h = acc[at, :].astype(BF16).astype(F32)
                gl_ref[...] += jnp.sum(d_h * hat, axis=0, keepdims=True)
                g = d_h * l_ref[...]
                d_x = rstd * (g - jnp.mean(g, axis=1, keepdims=True) - hat * jnp.mean(g * hat, axis=1, keepdims=True))
                o_ref[at, :] = (d_x + y_ref[at, :].astype(F32)).astype(BF16)

    whole = pl.BlockSpec((rows, d_model), lambda p, i: (0, 0))
    line = pl.BlockSpec((1, d_model), lambda p, i: (0, 0))
    return pl.pallas_call(
        kernel,
        grid=(3, steps),
        out_shape=[jax.ShapeDtypeStruct((rows, d_model), BF16), jax.ShapeDtypeStruct((1, d_model), F32)],
        in_specs=[pl.BlockSpec((group, width, rows), lambda p, i: (i, jnp.minimum(p, 1), 0)), pl.BlockSpec((group, width, rows), lambda p, i: (i, 0, 0)),
                  pl.BlockSpec((d_model, group * width), lambda p, i: (0, p * steps + i)), whole, line, whole],
        out_specs=[whole, line],
        scratch_shapes=[pltpu.VMEM((rows, d_model), F32)],
        compiler_params=pltpu.CompilerParams(vmem_limit_bytes=60 * 2 ** 20),
        cost_estimate=pl.CostEstimate(flops=6 * rows * d_model * d_model, bytes_accessed=6 * d_model * d_model, transcendentals=0),
        name='token_grads',
    )(tok_qk, tok_ov, w_qkv, x, ln_w, gy)


def token_cols(block, n_batch):
    return jnp.concatenate([block[8 * b:8 * b + 8, :].T for b in range(n_batch)], axis=0)


def qkv_heads(h_all, w_pad, stats, gains, n_dev, n_batch, tok, seq):
    rows = n_batch * tok
    d_model = h_all.shape[-1]
    n_h = gains.shape[0] // 2

    def kernel(h_ref, w_ref, st_ref, g_ref, q_ref, k_ref, v_ref, xq_ref, xk_ref):
        raw = jnp.dot(h_ref[...], w_ref[...], preferred_element_type=F32)
        st = token_cols(st_ref[0], n_batch)
        for n in range(n_h):
            for part, (o_ref, x_ref) in enumerate(((q_ref, xq_ref), (k_ref, xk_ref))):
                col = (part * n_h + n) * LANES
                hat = (raw[:, col:col + LANES] - st[:, 2 * part:2 * part + 1]) * st[:, 2 * part + 1:2 * part + 2]
                out = (hat * g_ref[part * n_h + n:part * n_h + n + 1, :]).astype(BF16)
                x_ref[:, n] = hat.reshape(n_batch, tok, LANES)
                o_ref[:, n] = out.reshape(n_batch, tok, LANES)
            col = (2 * n_h + n) * LANES
            v_ref[:, n] = raw[:, col:col + LANES].astype(BF16).reshape(n_batch, tok, LANES)

    shape = (n_batch, n_h, seq, LANES)
    spec = pl.BlockSpec((n_batch, n_h, tok, LANES), lambda i: (0, 0, i, 0))
    n_col = w_pad.shape[1]
    return pl.pallas_call(
        kernel,
        grid=(n_dev,),
        out_shape=[jax.ShapeDtypeStruct(shape, BF16)] * 3 + [jax.ShapeDtypeStruct(shape, F32)] * 2,
        in_specs=[pl.BlockSpec((rows, d_model), lambda i: (i, 0)), pl.BlockSpec((d_model, n_col), lambda i: (0, 0)),
                  pl.BlockSpec((1,) + stats.shape[1:], lambda i: (i, 0, 0)), pl.BlockSpec(gains.shape, lambda i: (0, 0))],
        out_specs=[spec] * 5,
        compiler_params=pltpu.CompilerParams(vmem_limit_bytes=60 * 2 ** 20),
        cost_estimate=pl.CostEstimate(flops=2 * n_dev * rows * d_model * n_col, bytes_accessed=80 * 2 ** 20, transcendentals=0),
        name='qkv_heads',
    )(h_all, w_pad, stats, gains)


def attention(q, k, v, d_o, hat_q, hat_k, gains, slopes, head_dim, blk):
    n_batch, n_h, seq, _ = q.shape
    n_blk = seq // blk
    tok = d_o.shape[-1] // n_batch
    n_grp = blk // tok
    scale = head_dim ** -0.5

    def dot(a, b):
        return jnp.dot(a, b, preferred_element_type=F32)

    def kernel(slope_ref, q_ref, k_ref, v_ref, do_ref, xq_ref, xk_ref, gq_ref, gk_ref, o_ref, dq_ref, dk_ref, dv_ref, sum_ref, gl_ref, w_ref, dk_acc, dv_acc, kt_ref, vt_ref):
        slope2 = slope_ref[pl.program_id(1)] * LOG2E
        dk_acc[...] = jnp.zeros_like(dk_acc)
        dv_acc[...] = jnp.zeros_like(dv_acc)
        kt_ref[...] = k_ref[0, 0].T
        vt_ref[...] = v_ref[0, 0].T
        sum_ref[...] = jnp.zeros_like(sum_ref)
        gl_ref[...] = jnp.zeros_like(gl_ref)

        def norm_terms(part, rows, d_b, x_ref, g_ref):
            gain = g_ref[0]
            prod = d_b.astype(F32) * x_ref[0, 0, rows, :]
            gl_ref[0, 0, part:part + 1, :] += jnp.sum(prod, axis=0, keepdims=True)
            prod = prod * gain
            pieces = [d_b]
            for _ in range(3):
                pieces.append(prod.astype(BF16))
                prod = prod - pieces[-1].astype(F32)
            row = lax.broadcasted_iota(jnp.int32, (8, LANES), 0)
            first = jnp.where(row == 0, jnp.broadcast_to(gain, (8, LANES)), 0.0).astype(BF16)
            other = jnp.where(row == 1, 1.0, 0.0).astype(BF16)
            lhs = jnp.concatenate([first, other, other, other], axis=1)
            both = lax.dot_general(lhs, jnp.concatenate(pieces, axis=1), (((1,), (1,)), ((), ())), preferred_element_type=F32)
            sum_ref[0, 0, 2 * part:2 * part + 2, rows] = both[:2]

        key_iota = lax.broadcasted_iota(jnp.int32, (blk, LANES), 0)[:, :1]
        blocks = [pl.ds(j * blk, blk) for j in range(n_blk)]

        for i in range(n_blk):
            q_b = q_ref[0, 0, blocks[i], :]
            q_t = q_b.T
            do_t = jnp.concatenate([do_ref[i * n_grp + m, 0] for m in range(n_grp)], axis=1)
            do_t = jnp.concatenate([do_t, jnp.zeros((LANES - head_dim, blk), BF16)], axis=0)
            do_b = do_t.T
            top = None
            for j in range(i, -1, -1):
                s = dot(k_ref[0, 0, blocks[j], :], q_t) * (scale * LOG2E)
                s = s + (key_iota + (j - i) * blk).astype(F32) * slope2
                if i == j:
                    key_pos = lax.broadcasted_iota(jnp.int32, (blk, blk), 0)
                    q_pos = lax.broadcasted_iota(jnp.int32, (blk, blk), 1)
                    s = jnp.where(key_pos <= q_pos, s, -1e30)
                w_ref[blocks[j], :] = s
                peak = jnp.max(s, axis=0, keepdims=True)
                top = peak if top is None else jnp.maximum(top, peak)

            total = jnp.zeros((1, blk), F32)
            out_t = jnp.zeros((LANES, blk), F32)
            for j in range(i + 1):
                w = jnp.exp2(w_ref[blocks[j], :] - top)
                w_ref[blocks[j], :] = w
                out_t = out_t + dot(vt_ref[:, blocks[j]], w.astype(BF16))
                total = total + jnp.sum(w, axis=0, keepdims=True)
            inv = 1.0 / total
            out_b = (out_t * inv).T.astype(BF16)
            o_ref[0, 0, blocks[i], :] = out_b
            delta = jnp.sum((out_b.astype(F32) * do_b.astype(F32)).T, axis=0, keepdims=True)

            dq_t = jnp.zeros((LANES, blk), F32)
            for j in range(i + 1):
                d_p = dot(v_ref[0, 0, blocks[j], :], do_t)
                p = w_ref[blocks[j], :] * inv
                dv_acc[blocks[j], :] += dot(p.astype(BF16), do_b)
                d_s = (p * (d_p - delta)).astype(BF16)
                dk_acc[blocks[j], :] += dot(d_s, q_b)
                dq_t = dq_t + dot(kt_ref[:, blocks[j]], d_s)
            dq_ref[0, 0, blocks[i], :] = (dq_t * scale).T.astype(BF16)

        @pl.loop(0, n_blk)
        def _(j):
            rows = pl.ds(pl.multiple_of(j * blk, blk), blk)
            dk_b = (dk_acc[rows, :] * scale).astype(BF16)
            dk_ref[0, 0, rows, :] = dk_b
            norm_terms(0, rows, dq_ref[0, 0, rows, :], xq_ref, gq_ref)
            norm_terms(1, rows, dk_b, xk_ref, gk_ref)

        dv_ref[0, 0] = dv_acc[...].astype(BF16)

    spec = pl.BlockSpec((1, 1, seq, LANES), lambda b, n: (b, n, 0, 0))
    flops = 6 * 2 * n_batch * n_h * seq * seq * LANES
    return pl.pallas_call(
        kernel,
        grid=(n_batch, n_h),
        out_shape=[jax.ShapeDtypeStruct(q.shape, BF16)] * 4 + [jax.ShapeDtypeStruct((n_batch, n_h, 8, n), F32) for n in (seq, LANES)],
        in_specs=[pl.BlockSpec(memory_space=pltpu.SMEM)] + [spec] * 3 + [pl.BlockSpec((seq // tok, 1, head_dim, tok), lambda b, n: (0, n, 0, b))] + [spec] * 2 + [pl.BlockSpec((1, 1, LANES), lambda b, n: (n, 0, 0)), pl.BlockSpec((1, 1, LANES), lambda b, n: (n_h + n, 0, 0))],
        out_specs=[spec] * 4 + [pl.BlockSpec((1, 1, 8, n), lambda b, n: (b, n, 0, 0)) for n in (seq, LANES)],
        scratch_shapes=[pltpu.VMEM((seq, blk), F32), pltpu.VMEM((seq, LANES), F32), pltpu.VMEM((seq, LANES), F32),
                        pltpu.VMEM((LANES, seq), BF16), pltpu.VMEM((LANES, seq), BF16)],
        compiler_params=pltpu.CompilerParams(vmem_limit_bytes=60 * 2 ** 20),
        cost_estimate=pl.CostEstimate(flops=flops, bytes_accessed=40 * 2 ** 20, transcendentals=n_batch * n_h * seq * seq // 2),
        name='attention',
    )(slopes, q, k, v, d_o, hat_q, hat_k, gains[:, None], gains[:, None])


def place_columns(buf, gathered, first, n_part, group, parts=1):
    n_dev, _, d_in = gathered.shape
    width = d_in // n_dev
    mb = 512 if d_in % 512 == 0 else d_in
    n_grp = n_dev // group

    def kernel(x_ref, *refs):
        refs[-1][...] = x_ref[...].reshape(group * width, mb).T

    args = (gathered,) if buf is None else (gathered, buf)
    return pl.pallas_call(
        kernel,
        grid=(parts, n_grp, d_in // mb),
        out_shape=jax.ShapeDtypeStruct((d_in, n_part * n_dev * width), gathered.dtype),
        in_specs=[pl.BlockSpec((group, width, mb), lambda p, g, m: (g, p, m))] + [pl.BlockSpec(memory_space=pl.ANY)] * (len(args) - 1),
        out_specs=pl.BlockSpec((mb, group * width), lambda p, g, m: (m, (p + first) * n_grp + g)),
        input_output_aliases={1: 0} if buf is not None else {},
        compiler_params=pltpu.CompilerParams(vmem_limit_bytes=40 * 2 ** 20),
        cost_estimate=pl.CostEstimate(flops=parts * d_in * d_in, bytes_accessed=8 * parts * d_in * d_in, transcendentals=0),
        name='place_columns',
    )(*args)


def place_rows(buf, gathered, first, n_rows, half, n_half):
    n_dev, _, d_in = gathered.shape
    group = math.gcd(n_dev, 4)

    def kernel(x_ref, *refs):
        refs[-1][:, 0] = x_ref[...]

    args = (gathered,) if buf is None else (gathered, buf)
    return pl.pallas_call(
        kernel,
        grid=(n_dev // group,),
        out_shape=jax.ShapeDtypeStruct((n_dev, n_half, n_rows, d_in), gathered.dtype),
        in_specs=[pl.BlockSpec((group, n_rows, d_in), lambda i: (i, first // n_rows, 0))] + [pl.BlockSpec(memory_space=pl.ANY)] * (len(args) - 1),
        out_specs=pl.BlockSpec((group, 1, n_rows, d_in), lambda i: (i, half, 0, 0)),
        input_output_aliases={1: 0} if buf is not None else {},
        compiler_params=pltpu.CompilerParams(vmem_limit_bytes=40 * 2 ** 20),
        cost_estimate=pl.CostEstimate(flops=n_dev * n_rows * d_in, bytes_accessed=8 * n_dev * n_rows * d_in, transcendentals=0),
        name='place_rows',
    )(*args)


def token_rows(arrays, n_dev, n_batch, tok, head_dim):
    n_h = arrays[0].shape[1]
    rows = n_batch * tok
    width = len(arrays) * n_h * head_dim

    def kernel(*refs):
        refs[-1][0] = jnp.concatenate([ref[:, n].reshape(rows, LANES).T[:head_dim] for ref in refs[:-1] for n in range(n_h)], axis=0)

    return pl.pallas_call(
        kernel,
        grid=(n_dev,),
        out_shape=jax.ShapeDtypeStruct((n_dev, width, rows), BF16),
        in_specs=[pl.BlockSpec((n_batch, n_h, tok, LANES), lambda i: (0, 0, i, 0))] * len(arrays),
        out_specs=pl.BlockSpec((1, width, rows), lambda i: (i, 0, 0)),
        cost_estimate=pl.CostEstimate(flops=n_dev * rows * width, bytes_accessed=4 * n_dev * rows * width, transcendentals=0),
        name='token_rows',
    )(*arrays)


def head_grads(side, acts, n_dev, n_batch, tok, head_dim):
    n_h = side.shape[1]
    rows, d_model = n_batch * tok, acts.shape[-1]

    def kernel(s_ref, a_ref, o_ref, acc):
        step = pl.program_id(0)
        lhs = jnp.concatenate([s_ref[:, n].reshape(rows, LANES) for n in range(n_h)], axis=1)

        @pl.when(step == 0)
        def _():
            acc[...] = jnp.zeros_like(acc)

        acc[...] += lax.dot_general(lhs, a_ref[...], (((0,), (0,)), ((), ())), preferred_element_type=F32)

        @pl.when(step == n_dev - 1)
        def _():
            for n in range(n_h):
                o_ref[n * head_dim:(n + 1) * head_dim, :] = acc[n * LANES:n * LANES + head_dim, :]

    return pl.pallas_call(
        kernel,
        grid=(n_dev,),
        out_shape=jax.ShapeDtypeStruct((n_h * head_dim, d_model), F32),
        in_specs=[pl.BlockSpec((n_batch, n_h, tok, LANES), lambda i: (0, 0, i, 0)), pl.BlockSpec((rows, d_model), lambda i: (i, 0))],
        out_specs=pl.BlockSpec((n_h * head_dim, d_model), lambda i: (0, 0)),
        scratch_shapes=[pltpu.VMEM((n_h * LANES, d_model), F32)],
        compiler_params=pltpu.CompilerParams(vmem_limit_bytes=50 * 2 ** 20),
        cost_estimate=pl.CostEstimate(flops=2 * n_dev * rows * d_model * n_h * LANES, bytes_accessed=50 * 2 ** 20, transcendentals=0),
        name='head_grads',
    )(side, acts)


def norm_back(d_q, d_k, hat_q, hat_k, stats, sums, gains, acts, n_dev, n_batch, tok, head_dim):
    n_h = d_q.shape[1]
    rows, d_model = n_batch * tok, acts.shape[-1]
    width = n_h * head_dim

    def kernel(dq_ref, dk_ref, xq_ref, xk_ref, st_ref, c_ref, g_ref, a_ref, w_ref, b_ref, acc):
        step = pl.program_id(0)
        st = token_cols(st_ref[0], n_batch)
        cols = token_cols(c_ref[0], n_batch)
        sides = []
        for part, (d_ref, x_ref) in enumerate(((dq_ref, xq_ref), (dk_ref, xk_ref))):
            r = st[:, 2 * part + 1:2 * part + 2]
            c1, c2 = (cols[:, 2 * part + m:2 * part + m + 1] for m in range(2))
            for n in range(n_h):
                g = d_ref[:, n].reshape(rows, LANES).astype(F32) * g_ref[part * n_h + n:part * n_h + n + 1, :]
                sides.append((r * (g - c1 - x_ref[:, n].reshape(rows, LANES) * c2)).astype(BF16))
        b_ref[0] = jnp.concatenate([a.T[:head_dim] for a in sides], axis=0)

        @pl.when(step == 0)
        def _():
            acc[...] = jnp.zeros_like(acc)

        acc[...] += lax.dot_general(jnp.concatenate(sides, axis=1), a_ref[...], (((0,), (0,)), ((), ())), preferred_element_type=F32)

        @pl.when(step == n_dev - 1)
        def _():
            for n in range(2 * n_h):
                w_ref[n * head_dim:(n + 1) * head_dim, :] = acc[n * LANES:n * LANES + head_dim, :]

    heads = pl.BlockSpec((n_batch, n_h, tok, LANES), lambda i: (0, 0, i, 0))
    return pl.pallas_call(
        kernel,
        grid=(n_dev,),
        out_shape=[jax.ShapeDtypeStruct((2 * width, d_model), F32), jax.ShapeDtypeStruct((n_dev, 2 * width, rows), BF16)],
        in_specs=[heads] * 4 + [pl.BlockSpec((1,) + stats.shape[1:], lambda i: (i, 0, 0))] * 2 + [pl.BlockSpec(gains.shape, lambda i: (0, 0)),
                                pl.BlockSpec((rows, d_model), lambda i: (i, 0))],
        out_specs=[pl.BlockSpec((2 * width, d_model), lambda i: (0, 0)), pl.BlockSpec((1, 2 * width, rows), lambda i: (i, 0, 0))],
        scratch_shapes=[pltpu.VMEM((2 * n_h * LANES, d_model), F32)],
        compiler_params=pltpu.CompilerParams(vmem_limit_bytes=60 * 2 ** 20),
        cost_estimate=pl.CostEstimate(flops=4 * n_dev * rows * d_model * n_h * LANES, bytes_accessed=90 * 2 ** 20, transcendentals=0),
        name='norm_back',
    )(d_q, d_k, hat_q, hat_k, stats, sums, gains, acts)


def solution(mesh):
    n_dev = mesh.shape['sp']
    seq_spec = P(None, 'sp', None)
    rep_spec = P()

    def local_step(x, ln1_w, w_qkv, q_ln_w, k_ln_w, w_out, grad_y):
        n_batch, tok, d_model = x.shape
        n_heads, head_dim = q_ln_w.shape
        n_h = n_heads // n_dev
        width = n_h * head_dim
        seq = tok * n_dev
        rows = n_batch * tok
        me = lax.axis_index('sp')
        slopes = lax.dynamic_slice_in_dim(alibi_slopes(n_heads), me * n_h, n_h)

        def pad_lanes(a):
            return jnp.pad(a, ((0, 0),) * (a.ndim - 1) + ((0, LANES - head_dim),))

        gy = grad_y.reshape(rows, d_model)
        h_loc = norm_rows(x.reshape(rows, d_model), ln1_w.astype(F32).reshape(1, d_model), math.gcd(rows, 128))
        h_all = lax.all_gather(h_loc, 'sp', axis=0, tiled=True)

        stats_loc = column_stats(h_loc, w_qkv, d_model // 4)[:, :, :2].reshape(2, n_batch, tok, 2)
        stats_loc = stats_loc.transpose(1, 0, 3, 2).reshape(n_batch, 4, tok)
        stats_loc = jnp.pad(stats_loc, ((0, 0), (0, 4), (0, 0))).reshape(8 * n_batch, tok)
        stats = exchange(stats_loc, n_dev)
        d_o = columns_of(w_out, gy, 4 * width).reshape(n_dev, width, rows)
        d_o, h_all = lax.optimization_barrier((d_o, h_all))
        d_o = lax.all_to_all(d_o, 'sp', 0, 0, tiled=True)
        d_o = d_o.reshape(n_dev, n_h, head_dim, rows)
        slices = [lax.dynamic_slice_in_dim(w_qkv, p * d_model + me * width, width, axis=1) for p in range(3)]
        w_pad = jnp.concatenate([pad_lanes(s[:, n * head_dim:(n + 1) * head_dim]) for s in slices for n in range(n_h)], axis=1)
        gain_q = pad_lanes(lax.dynamic_slice_in_dim(q_ln_w, me * n_h, n_h).astype(F32))
        gain_k = pad_lanes(lax.dynamic_slice_in_dim(k_ln_w, me * n_h, n_h).astype(F32))
        gains = jnp.concatenate([gain_q, gain_k])

        gy_late, stats = lax.optimization_barrier((gy, stats))
        gy_all = lax.all_gather(gy_late, 'sp', axis=0, tiled=True)
        q, k, v, hat_q, hat_k = qkv_heads(h_all, w_pad, stats, gains, n_dev, n_batch, tok, seq)
        o, d_q, d_k, d_v, head_sums, head_ln = attention(q, k, v, d_o, hat_q, hat_k, gains, slopes, head_dim, math.gcd(seq, 512))

        def gathered(a):
            return lax.all_gather(a, 'sp', axis=0, tiled=True)

        dw_v = head_grads(d_v, h_all, n_dev, n_batch, tok, head_dim)
        dw_v, d_q, d_k, head_sums = lax.optimization_barrier((dw_v, d_q, d_k, head_sums))
        dw_v = gathered(dw_v)

        part = jnp.sum(head_sums, axis=1).reshape(n_batch, 8, n_dev, tok).transpose(2, 0, 1, 3).reshape(n_dev, 8 * n_batch, tok)
        grad_q_ln, grad_k_ln = jnp.sum(head_ln, axis=0)[:, :2, :head_dim].transpose(1, 0, 2)
        part = exchange(part, n_dev, scatter=True)
        sums = exchange(jnp.sum(part, axis=0) * (1.0 / d_model), n_dev)

        d_v, o, sums = lax.optimization_barrier((d_v, o, sums))
        tok_ov = lax.all_to_all(token_rows((d_v, o), n_dev, n_batch, tok, head_dim), 'sp', 0, 0, tiled=True)
        dw_qk, back_qk = norm_back(d_q, d_k, hat_q, hat_k, stats, sums, gains, h_all, n_dev, n_batch, tok, head_dim)
        tok_qk = lax.all_to_all(back_qk, 'sp', 0, 0, tiled=True)
        o_late, dw_qk = lax.optimization_barrier((o, dw_qk))
        dw_out = head_grads(o_late, gy_all, n_dev, n_batch, tok, head_dim)
        half = width // 2
        dw_qko = gathered(jnp.concatenate([dw_qk, dw_out[:half]])).reshape(n_dev, 2 * width + half, d_model)
        dw_last = gathered(dw_out[half:]).reshape(n_dev, half, d_model)
        grad_w_qkv = place_columns(None, dw_v.reshape(n_dev, width, d_model), 2, 3, 4)
        grad_w_qkv = place_columns(grad_w_qkv, dw_qko, 0, 3, 4, parts=2)
        grad_w_out = place_rows(None, dw_qko, 2 * width, half, 0, 2)
        grad_w_out = place_rows(grad_w_out, dw_last, 0, half, 1, 2).reshape(d_model, d_model)

        x_rows = x.reshape(rows, d_model)
        y = project_out(tok_ov, w_out, x_rows, 4)
        grad_x, grad_ln1 = token_grads(tok_qk, tok_ov, w_qkv, x_rows, ln1_w.astype(F32).reshape(1, d_model), gy, 4, math.gcd(rows, 64))

        small = jnp.concatenate([grad_ln1[0], grad_q_ln.reshape(-1), grad_k_ln.reshape(-1)])
        n_small = small.shape[0]
        pad = -n_small % (8 * LANES)
        small_all = exchange(jnp.pad(small, (0, pad)).reshape(-1, LANES), n_dev).reshape(n_dev, n_small + pad)
        grad_ln1 = jnp.sum(small_all[:, :d_model], axis=0)
        grad_q_ln = small_all[:, d_model:d_model + width].reshape(n_heads, head_dim)
        grad_k_ln = small_all[:, d_model + width:d_model + 2 * width].reshape(n_heads, head_dim)
        shape = (n_batch, tok, d_model)
        return y.reshape(shape), grad_x.reshape(shape), grad_ln1, grad_w_qkv, grad_q_ln, grad_k_ln, grad_w_out

    return jax.shard_map(local_step, mesh=mesh, in_specs=(seq_spec, rep_spec, rep_spec, rep_spec, rep_spec, rep_spec, seq_spec), out_specs=(seq_spec, seq_spec, rep_spec, rep_spec, rep_spec, rep_spec, rep_spec), check_vma=False)
```

```python
import math
import jax
import jax.numpy as jnp
from jax import lax
from jax.experimental import pallas as pl
from jax.experimental.pallas import tpu as pltpu
from jax.sharding import PartitionSpec as P

F32 = jnp.float32
BF16 = jnp.bfloat16
LANES = 128
LOG2E = math.log2(math.e)
MESH = pl.DeviceIdType.MESH


def alibi_slopes(n_heads):
    pow_two = 2 ** math.ceil(math.log2(n_heads))
    exponents = jnp.arange(1, pow_two + 1, dtype=F32) * (8.0 / pow_two)
    slopes = jnp.exp2(-exponents)
    if pow_two != n_heads:
        slopes = jnp.concatenate([slopes[1::2], slopes[0::2]])[:n_heads]
    return slopes


def layer_norm(values, weight):
    centered = values - jnp.mean(values, axis=-1, keepdims=True)
    var_val = jnp.mean(centered * centered, axis=-1, keepdims=True)
    return centered * lax.rsqrt(var_val + 1e-5) * weight


def exchange(block, n_dev, scatter=False):
    shape = block.shape[1:] if scatter else block.shape

    def kernel(x_ref, o_ref, loc_sem, send_sem, recv_sem):
        me = lax.axis_index('sp')
        src = (lambda dev: x_ref.at[dev]) if scatter else (lambda dev: x_ref)
        own = pltpu.make_async_copy(src(me), o_ref.at[me], loc_sem)
        own.start()

        def copy(step):
            peer = lax.rem(me + step, n_dev)
            return pltpu.make_async_remote_copy(
                src_ref=src(peer), dst_ref=o_ref.at[me], send_sem=send_sem.at[step], recv_sem=recv_sem.at[step],
                device_id=(peer,), device_id_type=MESH)

        @pl.loop(1, n_dev)
        def _(step):
            copy(step).start()

        own.wait()

        @pl.loop(1, n_dev)
        def _(step):
            copy(step).wait()

    return pl.pallas_call(
        kernel,
        out_shape=jax.ShapeDtypeStruct((n_dev,) + shape, block.dtype),
        in_specs=[pl.BlockSpec(memory_space=pl.ANY)],
        out_specs=pl.BlockSpec(memory_space=pl.ANY),
        scratch_shapes=[pltpu.SemaphoreType.DMA, pltpu.SemaphoreType.DMA((n_dev,)), pltpu.SemaphoreType.DMA((n_dev,))],
        compiler_params=pltpu.CompilerParams(has_side_effects=True),
        name='scatter_rows' if scatter else 'exchange',
    )(block)


def norm_rows(x, weight, blk):
    rows, d_model = x.shape

    def kernel(x_ref, w_ref, o_ref):
        o_ref[...] = layer_norm(x_ref[...].astype(F32), w_ref[...]).astype(BF16)

    return pl.pallas_call(
        kernel,
        grid=(rows // blk,),
        out_shape=jax.ShapeDtypeStruct(x.shape, BF16),
        in_specs=[pl.BlockSpec((blk, d_model), lambda i: (i, 0)), pl.BlockSpec((1, d_model), lambda i: (0, 0))],
        out_specs=pl.BlockSpec((blk, d_model), lambda i: (i, 0)),
        cost_estimate=pl.CostEstimate(flops=8 * rows * d_model, bytes_accessed=4 * rows * d_model, transcendentals=0),
        name='norm_rows',
    )(x, weight)


def columns_of(weight, rows_in, blk):
    n_out, d_in = weight.shape
    rows = rows_in.shape[0]

    def kernel(w_ref, r_ref, o_ref):
        o_ref[...] = lax.dot_general(w_ref[...], r_ref[...], (((1,), (1,)), ((), ())), preferred_element_type=F32).astype(BF16)

    return pl.pallas_call(
        kernel,
        grid=(n_out // blk,),
        out_shape=jax.ShapeDtypeStruct((n_out, rows), BF16),
        in_specs=[pl.BlockSpec((blk, d_in), lambda i: (i, 0)), pl.BlockSpec((rows, d_in), lambda i: (0, 0))],
        out_specs=pl.BlockSpec((blk, rows), lambda i: (i, 0)),
        compiler_params=pltpu.CompilerParams(vmem_limit_bytes=40 * 2 ** 20),
        cost_estimate=pl.CostEstimate(flops=2 * n_out * d_in * rows, bytes_accessed=2 * (n_out + rows) * d_in, transcendentals=0),
        name='columns_of',
    )(weight, rows_in)


def column_stats(h, w_qkv, blk):
    rows, d_model = h.shape
    n_blk = d_model // blk

    def kernel(h_ref, w_ref, o_ref, raw):
        c = pl.program_id(1)
        raw[c] = jnp.dot(h_ref[...], w_ref[...], preferred_element_type=F32)

        @pl.when(c == n_blk - 1)
        def _():
            mean = sum(jnp.sum(raw[m], axis=1, keepdims=True) for m in range(n_blk)) * (1.0 / d_model)
            sq = jnp.zeros((rows, 1), F32)
            for m in range(n_blk):
                centered = raw[m] - mean
                sq = sq + jnp.sum(centered * centered, axis=1, keepdims=True)
            rstd = lax.rsqrt(sq * (1.0 / d_model) + 1e-5)
            lane = lax.broadcasted_iota(jnp.int32, (rows, LANES), 1)
            o_ref[0] = jnp.where(lane == 0, mean, rstd)

    return pl.pallas_call(
        kernel,
        grid=(2, n_blk),
        out_shape=jax.ShapeDtypeStruct((2, rows, LANES), F32),
        in_specs=[pl.BlockSpec((rows, d_model), lambda p, c: (0, 0)), pl.BlockSpec((d_model, blk), lambda p, c: (0, p * n_blk + c))],
        out_specs=pl.BlockSpec((1, rows, LANES), lambda p, c: (p, 0, 0)),
        scratch_shapes=[pltpu.VMEM((n_blk, rows, blk), F32)],
        compiler_params=pltpu.CompilerParams(vmem_limit_bytes=50 * 2 ** 20),
        cost_estimate=pl.CostEstimate(flops=4 * rows * d_model * d_model, bytes_accessed=4 * d_model * d_model, transcendentals=0),
        name='column_stats',
    )(h, w_qkv)


def project_out(tok_ov, w_out, x, group):
    rows, d_model = x.shape
    n_dev, width = tok_ov.shape[0], tok_ov.shape[1] // 2
    steps = n_dev // group

    def kernel(o_ref, w_ref, x_ref, y_ref, acc):
        step = pl.program_id(0)

        @pl.when(step == 0)
        def _():
            acc[...] = x_ref[...].astype(F32)

        acc[...] += lax.dot_general(o_ref[...].reshape(group * width, rows), w_ref[...], (((0,), (0,)), ((), ())), preferred_element_type=F32)

        @pl.when(step == steps - 1)
        def _():
            y_ref[...] = acc[...].astype(BF16)

    return pl.pallas_call(
        kernel,
        grid=(steps,),
        out_shape=jax.ShapeDtypeStruct((rows, d_model), BF16),
        in_specs=[pl.BlockSpec((group, width, rows), lambda i: (i, 1, 0)), pl.BlockSpec((group * width, d_model), lambda i: (i, 0)),
                  pl.BlockSpec((rows, d_model), lambda i: (0, 0))],
        out_specs=pl.BlockSpec((rows, d_model), lambda i: (0, 0)),
        scratch_shapes=[pltpu.VMEM((rows, d_model), F32)],
        compiler_params=pltpu.CompilerParams(vmem_limit_bytes=50 * 2 ** 20),
        cost_estimate=pl.CostEstimate(flops=2 * rows * d_model * d_model, bytes_accessed=2 * d_model * d_model, transcendentals=0),
        name='project_out',
    )(tok_ov, w_out, x)


def token_grads(tok_qk, tok_ov, w_qkv, x, ln_w, gy, group, chunk):
    rows, d_model = x.shape
    n_dev, width = tok_ov.shape[0], tok_ov.shape[1] // 2
    steps = n_dev // group

    def kernel(qk_ref, v_ref, w_ref, x_ref, l_ref, y_ref, o_ref, gl_ref, acc):
        part, step = pl.program_id(0), pl.program_id(1)

        @pl.when((part == 0) & (step == 0))
        def _():
            acc[...] = jnp.zeros_like(acc)

        side = jnp.where(part == 2, v_ref[...], qk_ref[...]).reshape(group * width, rows)
        acc[...] += lax.dot_general(side, w_ref[...], (((0,), (1,)), ((), ())), preferred_element_type=F32)

        @pl.when((part == 2) & (step == steps - 1))
        def _():
            gl_ref[...] = jnp.zeros_like(gl_ref)

            @pl.loop(0, rows // chunk)
            def _(m):
                at = pl.ds(pl.multiple_of(m * chunk, chunk), chunk)
                xs = x_ref[at, :].astype(F32)
                centered = xs - jnp.mean(xs, axis=1, keepdims=True)
                rstd = lax.rsqrt(jnp.mean(centered * centered, axis=1, keepdims=True) + 1e-5)
                hat = centered * rstd
                d_h = acc[at, :].astype(BF16).astype(F32)
                gl_ref[...] += jnp.sum(d_h * hat, axis=0, keepdims=True)
                g = d_h * l_ref[...]
                d_x = rstd * (g - jnp.mean(g, axis=1, keepdims=True) - hat * jnp.mean(g * hat, axis=1, keepdims=True))
                o_ref[at, :] = (d_x + y_ref[at, :].astype(F32)).astype(BF16)

    whole = pl.BlockSpec((rows, d_model), lambda p, i: (0, 0))
    line = pl.BlockSpec((1, d_model), lambda p, i: (0, 0))
    return pl.pallas_call(
        kernel,
        grid=(3, steps),
        out_shape=[jax.ShapeDtypeStruct((rows, d_model), BF16), jax.ShapeDtypeStruct((1, d_model), F32)],
        in_specs=[pl.BlockSpec((group, width, rows), lambda p, i: (i, jnp.minimum(p, 1), 0)), pl.BlockSpec((group, width, rows), lambda p, i: (i, 0, 0)),
                  pl.BlockSpec((d_model, group * width), lambda p, i: (0, p * steps + i)), whole, line, whole],
        out_specs=[whole, line],
        scratch_shapes=[pltpu.VMEM((rows, d_model), F32)],
        compiler_params=pltpu.CompilerParams(vmem_limit_bytes=60 * 2 ** 20),
        cost_estimate=pl.CostEstimate(flops=6 * rows * d_model * d_model, bytes_accessed=6 * d_model * d_model, transcendentals=0),
        name='token_grads',
    )(tok_qk, tok_ov, w_qkv, x, ln_w, gy)


def token_cols(block, n_batch):
    return jnp.concatenate([block[8 * b:8 * b + 8, :].T for b in range(n_batch)], axis=0)


def qkv_heads(h_all, w_pad, stats, gains, n_dev, n_batch, tok, seq):
    rows = n_batch * tok
    d_model = h_all.shape[-1]
    n_h = gains.shape[0] // 2

    def kernel(h_ref, w_ref, st_ref, g_ref, q_ref, k_ref, v_ref, xq_ref, xk_ref):
        raw = jnp.dot(h_ref[...], w_ref[...], preferred_element_type=F32)
        st = token_cols(st_ref[0], n_batch)
        for n in range(n_h):
            for part, (o_ref, x_ref) in enumerate(((q_ref, xq_ref), (k_ref, xk_ref))):
                col = (part * n_h + n) * LANES
                hat = (raw[:, col:col + LANES] - st[:, 2 * part:2 * part + 1]) * st[:, 2 * part + 1:2 * part + 2]
                out = (hat * g_ref[part * n_h + n:part * n_h + n + 1, :]).astype(BF16)
                x_ref[:, n] = hat.reshape(n_batch, tok, LANES)
                o_ref[:, n] = out.reshape(n_batch, tok, LANES)
            col = (2 * n_h + n) * LANES
            v_ref[:, n] = raw[:, col:col + LANES].astype(BF16).reshape(n_batch, tok, LANES)

    shape = (n_batch, n_h, seq, LANES)
    spec = pl.BlockSpec((n_batch, n_h, tok, LANES), lambda i: (0, 0, i, 0))
    n_col = w_pad.shape[1]
    return pl.pallas_call(
        kernel,
        grid=(n_dev,),
        out_shape=[jax.ShapeDtypeStruct(shape, BF16)] * 3 + [jax.ShapeDtypeStruct(shape, F32)] * 2,
        in_specs=[pl.BlockSpec((rows, d_model), lambda i: (i, 0)), pl.BlockSpec((d_model, n_col), lambda i: (0, 0)),
                  pl.BlockSpec((1,) + stats.shape[1:], lambda i: (i, 0, 0)), pl.BlockSpec(gains.shape, lambda i: (0, 0))],
        out_specs=[spec] * 5,
        compiler_params=pltpu.CompilerParams(vmem_limit_bytes=60 * 2 ** 20),
        cost_estimate=pl.CostEstimate(flops=2 * n_dev * rows * d_model * n_col, bytes_accessed=80 * 2 ** 20, transcendentals=0),
        name='qkv_heads',
    )(h_all, w_pad, stats, gains)


def attention(q, k, v, d_o, hat_q, hat_k, gains, slopes, head_dim, blk):
    n_batch, n_h, seq, _ = q.shape
    n_blk = seq // blk
    tok = d_o.shape[-1] // n_batch
    n_grp = blk // tok
    scale = head_dim ** -0.5

    def dot(a, b):
        return jnp.dot(a, b, preferred_element_type=F32)

    def kernel(slope_ref, q_ref, k_ref, v_ref, do_ref, xq_ref, xk_ref, gq_ref, gk_ref, o_ref, dq_ref, dk_ref, dv_ref, sum_ref, gl_ref, w_ref, dk_acc, dv_acc, kt_ref, vt_ref):
        slope2 = slope_ref[pl.program_id(1)] * LOG2E
        dk_acc[...] = jnp.zeros_like(dk_acc)
        dv_acc[...] = jnp.zeros_like(dv_acc)
        kt_ref[...] = k_ref[0, 0].T
        vt_ref[...] = v_ref[0, 0].T
        sum_ref[...] = jnp.zeros_like(sum_ref)
        gl_ref[...] = jnp.zeros_like(gl_ref)

        def norm_terms(part, rows, d_b, x_ref, g_ref):
            gain = g_ref[0]
            prod = d_b.astype(F32) * x_ref[0, 0, rows, :]
            gl_ref[0, 0, part:part + 1, :] += jnp.sum(prod, axis=0, keepdims=True)
            prod = prod * gain * 0.0625
            pieces = [d_b]
            for _ in range(3):
                pieces.append(prod.astype(BF16))
                prod = prod - pieces[-1].astype(F32)
            row = lax.broadcasted_iota(jnp.int32, (8, LANES), 0)
            first = jnp.where(row == 0, jnp.broadcast_to(gain, (8, LANES)), 0.0).astype(BF16)
            other = jnp.where(row == 1, 1.0, 0.0).astype(BF16)
            lhs = jnp.concatenate([first, other, other, other], axis=1)
            both = lax.dot_general(lhs, jnp.concatenate(pieces, axis=1), (((1,), (1,)), ((), ())), preferred_element_type=F32)
            sum_ref[0, 0, 2 * part:2 * part + 1, rows] = both[:1]
            sum_ref[0, 0, 2 * part + 1:2 * part + 2, rows] = both[1:2] * 16.0

        key_iota = lax.broadcasted_iota(jnp.int32, (blk, LANES), 0)[:, :1]
        blocks = [pl.ds(j * blk, blk) for j in range(n_blk)]

        for i in range(n_blk):
            q_b = q_ref[0, 0, blocks[i], :]
            q_t = q_b.T
            do_t = jnp.concatenate([do_ref[i * n_grp + m, 0] for m in range(n_grp)], axis=1)
            do_t = jnp.concatenate([do_t, jnp.zeros((LANES - head_dim, blk), BF16)], axis=0)
            do_b = do_t.T
            top = None
            for j in range(i, -1, -1):
                s = dot(k_ref[0, 0, blocks[j], :], q_t) * (scale * LOG2E)
                s = s + (key_iota + (j - i) * blk).astype(F32) * slope2
                if i == j:
                    key_pos = lax.broadcasted_iota(jnp.int32, (blk, blk), 0)
                    q_pos = lax.broadcasted_iota(jnp.int32, (blk, blk), 1)
                    s = jnp.where(key_pos <= q_pos, s, -1e30)
                w_ref[blocks[j], :] = s
                peak = jnp.max(s, axis=0, keepdims=True)
                top = peak if top is None else jnp.maximum(top, peak)

            total = jnp.zeros((1, blk), F32)
            out_t = jnp.zeros((LANES, blk), F32)
            for j in range(i + 1):
                w = jnp.exp2(w_ref[blocks[j], :] - top)
                w_ref[blocks[j], :] = w
                out_t = out_t + dot(vt_ref[:, blocks[j]], w.astype(BF16))
                total = total + jnp.sum(w, axis=0, keepdims=True)
            inv = 1.0 / total
            out_b = (out_t * inv).T.astype(BF16)
            o_ref[0, 0, blocks[i], :] = out_b
            delta = jnp.sum((out_b.astype(F32) * do_b.astype(F32)).T, axis=0, keepdims=True)

            dq_t = jnp.zeros((LANES, blk), F32)
            for j in range(i + 1):
                d_p = dot(v_ref[0, 0, blocks[j], :], do_t)
                p = w_ref[blocks[j], :] * inv
                dv_acc[blocks[j], :] += dot(p.astype(BF16), do_b)
                d_s = (p * (d_p - delta)).astype(BF16)
                dk_acc[blocks[j], :] += dot(d_s, q_b)
                dq_t = dq_t + dot(kt_ref[:, blocks[j]], d_s)
            dq_ref[0, 0, blocks[i], :] = (dq_t * scale).T.astype(BF16)

        @pl.loop(0, n_blk)
        def _(j):
            rows = pl.ds(pl.multiple_of(j * blk, blk), blk)
            dk_b = (dk_acc[rows, :] * scale).astype(BF16)
            dk_ref[0, 0, rows, :] = dk_b
            norm_terms(0, rows, dq_ref[0, 0, rows, :], xq_ref, gq_ref)
            norm_terms(1, rows, dk_b, xk_ref, gk_ref)

        dv_ref[0, 0] = dv_acc[...].astype(BF16)

    spec = pl.BlockSpec((1, 1, seq, LANES), lambda b, n: (b, n, 0, 0))
    flops = 6 * 2 * n_batch * n_h * seq * seq * LANES
    return pl.pallas_call(
        kernel,
        grid=(n_batch, n_h),
        out_shape=[jax.ShapeDtypeStruct(q.shape, BF16)] * 4 + [jax.ShapeDtypeStruct((n_batch, n_h, 8, n), F32) for n in (seq, LANES)],
        in_specs=[pl.BlockSpec(memory_space=pltpu.SMEM)] + [spec] * 3 + [pl.BlockSpec((seq // tok, 1, head_dim, tok), lambda b, n: (0, n, 0, b))] + [spec] * 2 + [pl.BlockSpec((1, 1, LANES), lambda b, n: (n, 0, 0)), pl.BlockSpec((1, 1, LANES), lambda b, n: (n_h + n, 0, 0))],
        out_specs=[spec] * 4 + [pl.BlockSpec((1, 1, 8, n), lambda b, n: (b, n, 0, 0)) for n in (seq, LANES)],
        scratch_shapes=[pltpu.VMEM((seq, blk), F32), pltpu.VMEM((seq, LANES), F32), pltpu.VMEM((seq, LANES), F32),
                        pltpu.VMEM((LANES, seq), BF16), pltpu.VMEM((LANES, seq), BF16)],
        compiler_params=pltpu.CompilerParams(vmem_limit_bytes=60 * 2 ** 20),
        cost_estimate=pl.CostEstimate(flops=flops, bytes_accessed=40 * 2 ** 20, transcendentals=n_batch * n_h * seq * seq // 2),
        name='attention',
    )(slopes, q, k, v, d_o, hat_q, hat_k, gains[:, None], gains[:, None])


def place_columns(buf, gathered, first, n_part, group, parts=1):
    n_dev, _, d_in = gathered.shape
    width = d_in // n_dev
    mb = 512 if d_in % 512 == 0 else d_in
    n_grp = n_dev // group

    def kernel(x_ref, *refs):
        refs[-1][...] = x_ref[...].reshape(group * width, mb).T

    args = (gathered,) if buf is None else (gathered, buf)
    return pl.pallas_call(
        kernel,
        grid=(parts, n_grp, d_in // mb),
        out_shape=jax.ShapeDtypeStruct((d_in, n_part * n_dev * width), gathered.dtype),
        in_specs=[pl.BlockSpec((group, width, mb), lambda p, g, m: (g, p, m))] + [pl.BlockSpec(memory_space=pl.ANY)] * (len(args) - 1),
        out_specs=pl.BlockSpec((mb, group * width), lambda p, g, m: (m, (p + first) * n_grp + g)),
        input_output_aliases={1: 0} if buf is not None else {},
        compiler_params=pltpu.CompilerParams(vmem_limit_bytes=40 * 2 ** 20),
        cost_estimate=pl.CostEstimate(flops=parts * d_in * d_in, bytes_accessed=8 * parts * d_in * d_in, transcendentals=0),
        name='place_columns',
    )(*args)


def place_rows(buf, gathered, first, n_rows, half, n_half):
    n_dev, _, d_in = gathered.shape
    group = math.gcd(n_dev, 4)

    def kernel(x_ref, *refs):
        refs[-1][:, 0] = x_ref[...]

    args = (gathered,) if buf is None else (gathered, buf)
    return pl.pallas_call(
        kernel,
        grid=(n_dev // group,),
        out_shape=jax.ShapeDtypeStruct((n_dev, n_half, n_rows, d_in), gathered.dtype),
        in_specs=[pl.BlockSpec((group, n_rows, d_in), lambda i: (i, first // n_rows, 0))] + [pl.BlockSpec(memory_space=pl.ANY)] * (len(args) - 1),
        out_specs=pl.BlockSpec((group, 1, n_rows, d_in), lambda i: (i, half, 0, 0)),
        input_output_aliases={1: 0} if buf is not None else {},
        compiler_params=pltpu.CompilerParams(vmem_limit_bytes=40 * 2 ** 20),
        cost_estimate=pl.CostEstimate(flops=n_dev * n_rows * d_in, bytes_accessed=8 * n_dev * n_rows * d_in, transcendentals=0),
        name='place_rows',
    )(*args)


def token_rows(arrays, n_dev, n_batch, tok, head_dim):
    n_h = arrays[0].shape[1]
    rows = n_batch * tok
    width = len(arrays) * n_h * head_dim

    def kernel(*refs):
        refs[-1][0] = jnp.concatenate([ref[:, n].reshape(rows, LANES).T[:head_dim] for ref in refs[:-1] for n in range(n_h)], axis=0)

    return pl.pallas_call(
        kernel,
        grid=(n_dev,),
        out_shape=jax.ShapeDtypeStruct((n_dev, width, rows), BF16),
        in_specs=[pl.BlockSpec((n_batch, n_h, tok, LANES), lambda i: (0, 0, i, 0))] * len(arrays),
        out_specs=pl.BlockSpec((1, width, rows), lambda i: (i, 0, 0)),
        cost_estimate=pl.CostEstimate(flops=n_dev * rows * width, bytes_accessed=4 * n_dev * rows * width, transcendentals=0),
        name='token_rows',
    )(*arrays)


def head_grads(side, acts, n_dev, n_batch, tok, head_dim):
    n_h = side.shape[1]
    rows, d_model = n_batch * tok, acts.shape[-1]

    def kernel(s_ref, a_ref, o_ref, acc):
        step = pl.program_id(0)
        lhs = jnp.concatenate([s_ref[:, n].reshape(rows, LANES) for n in range(n_h)], axis=1)

        @pl.when(step == 0)
        def _():
            acc[...] = jnp.zeros_like(acc)

        acc[...] += lax.dot_general(lhs, a_ref[...], (((0,), (0,)), ((), ())), preferred_element_type=F32)

        @pl.when(step == n_dev - 1)
        def _():
            for n in range(n_h):
                o_ref[n * head_dim:(n + 1) * head_dim, :] = acc[n * LANES:n * LANES + head_dim, :]

    return pl.pallas_call(
        kernel,
        grid=(n_dev,),
        out_shape=jax.ShapeDtypeStruct((n_h * head_dim, d_model), F32),
        in_specs=[pl.BlockSpec((n_batch, n_h, tok, LANES), lambda i: (0, 0, i, 0)), pl.BlockSpec((rows, d_model), lambda i: (i, 0))],
        out_specs=pl.BlockSpec((n_h * head_dim, d_model), lambda i: (0, 0)),
        scratch_shapes=[pltpu.VMEM((n_h * LANES, d_model), F32)],
        compiler_params=pltpu.CompilerParams(vmem_limit_bytes=50 * 2 ** 20),
        cost_estimate=pl.CostEstimate(flops=2 * n_dev * rows * d_model * n_h * LANES, bytes_accessed=50 * 2 ** 20, transcendentals=0),
        name='head_grads',
    )(side, acts)


def norm_back(d_q, d_k, hat_q, hat_k, stats, sums, gains, acts, n_dev, n_batch, tok, head_dim):
    n_h = d_q.shape[1]
    rows, d_model = n_batch * tok, acts.shape[-1]
    width = n_h * head_dim

    def kernel(dq_ref, dk_ref, xq_ref, xk_ref, st_ref, c_ref, g_ref, a_ref, w_ref, b_ref, acc):
        step = pl.program_id(0)
        st = token_cols(st_ref[0], n_batch)
        cols = token_cols(c_ref[0], n_batch)
        sides = []
        for part, (d_ref, x_ref) in enumerate(((dq_ref, xq_ref), (dk_ref, xk_ref))):
            r = st[:, 2 * part + 1:2 * part + 2]
            c1, c2 = (cols[:, 2 * part + m:2 * part + m + 1] for m in range(2))
            for n in range(n_h):
                g = d_ref[:, n].reshape(rows, LANES).astype(F32) * g_ref[part * n_h + n:part * n_h + n + 1, :]
                sides.append((r * (g - c1 - x_ref[:, n].reshape(rows, LANES) * c2)).astype(BF16))
        b_ref[0] = jnp.concatenate([a.T[:head_dim] for a in sides], axis=0)

        @pl.when(step == 0)
        def _():
            acc[...] = jnp.zeros_like(acc)

        acc[...] += lax.dot_general(jnp.concatenate(sides, axis=1), a_ref[...], (((0,), (0,)), ((), ())), preferred_element_type=F32)

        @pl.when(step == n_dev - 1)
        def _():
            for n in range(2 * n_h):
                w_ref[n * head_dim:(n + 1) * head_dim, :] = acc[n * LANES:n * LANES + head_dim, :]

    heads = pl.BlockSpec((n_batch, n_h, tok, LANES), lambda i: (0, 0, i, 0))
    return pl.pallas_call(
        kernel,
        grid=(n_dev,),
        out_shape=[jax.ShapeDtypeStruct((2 * width, d_model), F32), jax.ShapeDtypeStruct((n_dev, 2 * width, rows), BF16)],
        in_specs=[heads] * 4 + [pl.BlockSpec((1,) + stats.shape[1:], lambda i: (i, 0, 0))] * 2 + [pl.BlockSpec(gains.shape, lambda i: (0, 0)),
                                pl.BlockSpec((rows, d_model), lambda i: (i, 0))],
        out_specs=[pl.BlockSpec((2 * width, d_model), lambda i: (0, 0)), pl.BlockSpec((1, 2 * width, rows), lambda i: (i, 0, 0))],
        scratch_shapes=[pltpu.VMEM((2 * n_h * LANES, d_model), F32)],
        compiler_params=pltpu.CompilerParams(vmem_limit_bytes=60 * 2 ** 20),
        cost_estimate=pl.CostEstimate(flops=4 * n_dev * rows * d_model * n_h * LANES, bytes_accessed=90 * 2 ** 20, transcendentals=0),
        name='norm_back',
    )(d_q, d_k, hat_q, hat_k, stats, sums, gains, acts)


def solution(mesh):
    n_dev = mesh.shape['sp']
    seq_spec = P(None, 'sp', None)
    rep_spec = P()

    def local_step(x, ln1_w, w_qkv, q_ln_w, k_ln_w, w_out, grad_y):
        n_batch, tok, d_model = x.shape
        n_heads, head_dim = q_ln_w.shape
        n_h = n_heads // n_dev
        width = n_h * head_dim
        seq = tok * n_dev
        rows = n_batch * tok
        me = lax.axis_index('sp')
        slopes = lax.dynamic_slice_in_dim(alibi_slopes(n_heads), me * n_h, n_h)

        def pad_lanes(a):
            return jnp.pad(a, ((0, 0),) * (a.ndim - 1) + ((0, LANES - head_dim),))

        gy = grad_y.reshape(rows, d_model)
        h_loc = norm_rows(x.reshape(rows, d_model), ln1_w.astype(F32).reshape(1, d_model), math.gcd(rows, 128))
        h_all = lax.all_gather(h_loc, 'sp', axis=0, tiled=True)

        stats_loc = column_stats(h_loc, w_qkv, d_model // 4)[:, :, :2].reshape(2, n_batch, tok, 2)
        stats_loc = stats_loc.transpose(1, 0, 3, 2).reshape(n_batch, 4, tok)
        stats_loc = jnp.pad(stats_loc, ((0, 0), (0, 4), (0, 0))).reshape(8 * n_batch, tok)
        stats = exchange(stats_loc, n_dev)
        d_o = columns_of(w_out, gy, 4 * width).reshape(n_dev, width, rows)
        d_o, h_all = lax.optimization_barrier((d_o, h_all))
        d_o = lax.all_to_all(d_o, 'sp', 0, 0, tiled=True)
        d_o = d_o.reshape(n_dev, n_h, head_dim, rows)
        slices = [lax.dynamic_slice_in_dim(w_qkv, p * d_model + me * width, width, axis=1) for p in range(3)]
        w_pad = jnp.concatenate([pad_lanes(s[:, n * head_dim:(n + 1) * head_dim]) for s in slices for n in range(n_h)], axis=1)
        gain_q = pad_lanes(lax.dynamic_slice_in_dim(q_ln_w, me * n_h, n_h).astype(F32))
        gain_k = pad_lanes(lax.dynamic_slice_in_dim(k_ln_w, me * n_h, n_h).astype(F32))
        gains = jnp.concatenate([gain_q, gain_k])

        gy_late, stats = lax.optimization_barrier((gy, stats))
        gy_all = lax.all_gather(gy_late, 'sp', axis=0, tiled=True)
        q, k, v, hat_q, hat_k = qkv_heads(h_all, w_pad, stats, gains, n_dev, n_batch, tok, seq)
        o, d_q, d_k, d_v, head_sums, head_ln = attention(q, k, v, d_o, hat_q, hat_k, gains, slopes, head_dim, math.gcd(seq, 512))

        def gathered(a):
            return lax.all_gather(a, 'sp', axis=0, tiled=True)

        dw_v = head_grads(d_v, h_all, n_dev, n_batch, tok, head_dim)
        dw_v, d_q, d_k, head_sums = lax.optimization_barrier((dw_v, d_q, d_k, head_sums))
        dw_v = gathered(dw_v)

        part = jnp.sum(head_sums, axis=1).reshape(n_batch, 8, n_dev, tok).transpose(2, 0, 1, 3).reshape(n_dev, 8 * n_batch, tok)
        grad_q_ln, grad_k_ln = jnp.sum(head_ln, axis=0)[:, :2, :head_dim].transpose(1, 0, 2)
        part = exchange(part, n_dev, scatter=True)
        sums = exchange(jnp.sum(part, axis=0) * (1.0 / d_model), n_dev)

        d_v, o, sums = lax.optimization_barrier((d_v, o, sums))
        tok_ov = lax.all_to_all(token_rows((d_v, o), n_dev, n_batch, tok, head_dim), 'sp', 0, 0, tiled=True)
        dw_qk, back_qk = norm_back(d_q, d_k, hat_q, hat_k, stats, sums, gains, h_all, n_dev, n_batch, tok, head_dim)
        tok_qk = lax.all_to_all(back_qk, 'sp', 0, 0, tiled=True)
        o_late, dw_qk = lax.optimization_barrier((o, dw_qk))
        dw_out = head_grads(o_late, gy_all, n_dev, n_batch, tok, head_dim)
        half = width // 2
        dw_qko = gathered(jnp.concatenate([dw_qk, dw_out[:half]])).reshape(n_dev, 2 * width + half, d_model)
        dw_last = gathered(dw_out[half:]).reshape(n_dev, half, d_model)
        grad_w_qkv = place_columns(None, dw_v.reshape(n_dev, width, d_model), 2, 3, 4)
        grad_w_qkv = place_columns(grad_w_qkv, dw_qko, 0, 3, 4, parts=2)
        grad_w_out = place_rows(None, dw_qko, 2 * width, half, 0, 2)
        grad_w_out = place_rows(grad_w_out, dw_last, 0, half, 1, 2).reshape(d_model, d_model)

        x_rows = x.reshape(rows, d_model)
        y = project_out(tok_ov, w_out, x_rows, 4)
        grad_x, grad_ln1 = token_grads(tok_qk, tok_ov, w_qkv, x_rows, ln1_w.astype(F32).reshape(1, d_model), gy, 4, math.gcd(rows, 64))

        small = jnp.concatenate([grad_ln1[0], grad_q_ln.reshape(-1), grad_k_ln.reshape(-1)])
        n_small = small.shape[0]
        pad = -n_small % (8 * LANES)
        small_all = exchange(jnp.pad(small, (0, pad)).reshape(-1, LANES), n_dev).reshape(n_dev, n_small + pad)
        grad_ln1 = jnp.sum(small_all[:, :d_model], axis=0)
        grad_q_ln = small_all[:, d_model:d_model + width].reshape(n_heads, head_dim)
        grad_k_ln = small_all[:, d_model + width:d_model + 2 * width].reshape(n_heads, head_dim)
        shape = (n_batch, tok, d_model)
        return y.reshape(shape), grad_x.reshape(shape), grad_ln1, grad_w_qkv, grad_q_ln, grad_k_ln, grad_w_out

    return jax.shard_map(local_step, mesh=mesh, in_specs=(seq_spec, rep_spec, rep_spec, rep_spec, rep_spec, rep_spec, seq_spec), out_specs=(seq_spec, seq_spec, rep_spec, rep_spec, rep_spec, rep_spec, rep_spec), check_vma=False)
```
